32 devices in a mesh: dp: 4 (over y, x), tensor: 8 (over z, core).
Axes of the slice: x: 2, y: 2, z: 4, core: 2. Of those that a mesh axis runs over, the one named last changes fastest.
Arguments:
- saved_input: bfloat16 [512, 8192], P(('dp', 'tensor')), may hold values from -8 to 8
- keep_bits: int32 [512, 448], P(('dp', 'tensor')), may hold values from -2147483648 to 2147483646, as said below
- norm_gain: bfloat16 [8192], P('dp'), may hold values from 0.099609375 to 1.8984375
- gate_weight: bfloat16 [8192, 14336], P('dp', 'tensor'), may hold values from -0.0625 to 0.0625
- up_weight: bfloat16 [8192, 14336], P('dp', 'tensor'), may hold values from -0.0625 to 0.0625
- down_weight: bfloat16 [14336, 8192], P('tensor', 'dp'), may hold values from -0.046875 to 0.046875
Outputs:
- layer_out: bfloat16 [512, 8192], P('tensor', 'dp')
- row_check: float32 [512], P('tensor')
The draws below stay inside these ranges and needn't reach their ends.
Inputs may be any that keep to these rules, and one draw needn't show every extreme that they name: `keep_bits`: bit k of word w of a token is the keep bit of hidden unit 32 w + k.
All inputs are finite; a program needn't handle non-finite values.
Results may differ from the reference program's by a relative error of at most 0.017.
Values may be sent and summed in bfloat16 or wider, within the bound.
A program may use at most 64 MiB of HBM per device.

```python
import jax
import jax.numpy as jnp
from jax import lax

D = 8192
FF = 14336
TOKENS = 512
WORDS = 448


def draw_saved_input(key, part):
    keys = jax.random.split(jax.random.fold_in(key, 11), 2)
    base = jax.random.normal(keys[0], (TOKENS, D), jnp.float32)
    rough = jnp.exp(jax.random.uniform(keys[1], (1, D), jnp.float32, -0.35, 0.35))
    rising = jnp.exp(jnp.linspace(-0.55, 0.55, D, dtype=jnp.float32))[None, :]
    values = base * rough * rising
    return jnp.clip(values, -8.0, 8.0).astype(jnp.bfloat16)


def draw_keep_bits(key, part):
    return jax.random.randint(jax.random.fold_in(key, 23), (TOKENS, WORDS), -2147483648, 2147483647, jnp.int32)


def block_levels(own_key, shape, shards, low, high):
    def one(dim, parts):
        heights = jax.random.uniform(jax.random.fold_in(jax.random.fold_in(own_key, 6), dim), (parts,), jnp.float32, low / len(shards), high / len(shards))
        return jnp.repeat(jnp.exp(heights), shape[dim] // parts).reshape((-1,) + (1,) * (len(shape) - dim - 1))

    gain = one(*shards[0])
    for cut in shards[1:]:
        gain = gain * one(*cut)
    return gain


def scatter_about(stream_key, dims, deviation, most, cuts=(), kind=jnp.bfloat16):
    level = block_levels(stream_key, dims, cuts, -0.22, 0.18) if cuts else 1.0
    result = jax.random.normal(stream_key, dims, jnp.float32) * deviation * level
    return jnp.minimum(jnp.maximum(result, -most), most).astype(kind)


def setup_inputs(seed: int = 0) -> dict:
    arg_keys = jax.random.split(jax.random.key(seed), 7)
    return {
        "saved_input": draw_saved_input(jax.random.fold_in(arg_keys[6], 71), 0),
        "keep_bits": draw_keep_bits(jax.random.fold_in(arg_keys[6], 71), 0),
        "norm_gain": jnp.clip(1.0 + 0.18 * jax.random.normal(arg_keys[2], (D,), jnp.float32), 0.099609375, 1.8984375).astype(jnp.bfloat16),
        "gate_weight": scatter_about(arg_keys[3], (D, FF), D ** -0.5, 0.0625, ((0, 4), (1, 8))),
        "up_weight": scatter_about(arg_keys[4], (D, FF), D ** -0.5, 0.0625, ((0, 4), (1, 8))),
        "down_weight": scatter_about(arg_keys[5], (FF, D), FF ** -0.5, 0.046875, ((0, 8), (1, 4))),
    }


def reference(saved_input, keep_bits, norm_gain, gate_weight, up_weight, down_weight):
    widened = saved_input.astype(jnp.float32)
    inv_rms = lax.rsqrt(lax.optimization_barrier(jnp.sum(widened * widened, axis=1, keepdims=True)) / D + 1e-05)
    normed = (widened * inv_rms * norm_gain.astype(jnp.float32)).astype(jnp.bfloat16)
    gate = jnp.dot(normed, gate_weight, preferred_element_type=jnp.float32)
    up_sum = jnp.dot(normed, up_weight, preferred_element_type=jnp.float32)
    shifts = jnp.arange(32, dtype=jnp.int32)
    keep_mask = jnp.bitwise_and(jnp.right_shift(keep_bits[:, :, None], shifts[None, None, :]), 1)
    keep_mask = keep_mask.reshape(keep_bits.shape[0], -1)
    hidden = (jax.nn.silu(gate) * up_sum * (2.0 * keep_mask.astype(jnp.float32))).astype(jnp.bfloat16)
    layer_out = (widened + jnp.dot(hidden, down_weight, preferred_element_type=jnp.float32)).astype(jnp.bfloat16)
    widened_out = layer_out.astype(jnp.float32)
    row_check = lax.optimization_barrier(jnp.sum(widened_out * widened_out, axis=1)) / D
    return (layer_out, row_check)
```

```python
import jax
import jax.numpy as jnp
from jax import lax
from jax.experimental import pallas as pl
from jax.experimental.pallas import tpu as pltpu
from jax.sharding import PartitionSpec as P

D = 8192


def on_device(saved_input, keep_bits, norm_gain, gate_weight, up_weight, down_weight):
    tensor_width = lax.axis_size("tensor")
    dp_width = lax.axis_size("dp")
    unit_words = lax.all_to_all(keep_bits, "tensor", split_axis=1, concat_axis=0, tiled=True)
    shifts = jnp.arange(32, dtype=jnp.int32)
    keep_mask = jnp.bitwise_and(jnp.right_shift(unit_words[:, :, None], shifts[None, None, :]), 1)
    keep_mask = keep_mask.reshape(unit_words.shape[0], -1)
    keep_scale = 2.0 * keep_mask.astype(jnp.float32)
    width_units = gate_weight.shape[1]
    columns = lax.all_to_all(saved_input, "dp", split_axis=1, concat_axis=0, tiled=True)
    collected = lax.all_gather(columns, "tensor", axis=0, tiled=True)
    per_device = saved_input.shape[0]
    collected = collected.reshape(tensor_width, dp_width, per_device, collected.shape[1])
    collected = collected.transpose(1, 0, 2, 3).reshape(-1, collected.shape[3])
    widened = collected.astype(jnp.float32)
    squares = lax.psum(jnp.sum(widened * widened, axis=1), "dp")
    inv_rms = lax.rsqrt(squares / D + 1e-05)
    normed = (widened * inv_rms[:, None] * norm_gain.astype(jnp.float32)[None, :]).astype(
        jnp.bfloat16
    )
    gate_part = jnp.dot(normed, gate_weight, preferred_element_type=jnp.float32)
    up_part = jnp.dot(normed, up_weight, preferred_element_type=jnp.float32)
    projected = lax.psum_scatter(
        jnp.concatenate((gate_part, up_part), axis=1).astype(jnp.bfloat16),
        "dp",
        scatter_dimension=0,
        tiled=True,
    ).astype(jnp.float32)
    gate_sum = projected[:, :width_units]
    up_sum = projected[:, width_units:]
    hidden = (jax.nn.silu(gate_sum) * up_sum * keep_scale).astype(jnp.bfloat16)
    partial_value = jnp.dot(
        lax.all_gather(hidden, "dp", axis=0, tiled=True),
        down_weight,
        preferred_element_type=jnp.float32,
    )
    mlp_sum = lax.psum_scatter(
        partial_value.astype(jnp.bfloat16), "tensor", scatter_dimension=0, tiled=True
    ).astype(jnp.float32)
    out_rows = mlp_sum.shape[0]
    first_row = lax.axis_index("tensor") * out_rows
    residual = lax.dynamic_slice_in_dim(collected, first_row, out_rows, 0)
    layer_out = (residual.astype(jnp.float32) + mlp_sum).astype(jnp.bfloat16)
    widened_out = layer_out.astype(jnp.float32)
    row_check = lax.psum(jnp.sum(widened_out * widened_out, axis=1), "dp") / D
    return (layer_out, row_check)


MESH = pl.DeviceIdType.MESH
F32 = jnp.float32
BF16 = jnp.bfloat16
WAVES = 4
COL_PARTS = 2


SCHEDULE = (
    ("own", 0), ("own", 1), ("ring", 0, 1), ("ring", 0, 2), ("ring", 0, 0), ("own", 2), ("gather", 0),
    ("project", 0, 0), ("ring", 1, 2), ("project", 0, 1), ("ring", 1, 1), ("ring", 1, 0), ("relay", 0, 0, 1),
    ("bits",), ("relay", 0, 0, 0), ("gather", 1), ("project", 1, 1), ("relay", 0, 1, 0), ("project", 1, 0),
    ("relay", 0, 1, 1), ("ring", 2, 1), ("ring", 2, 2), ("relay", 1, 1, 0), ("relay", 1, 1, 1), ("expand",),
    ("own", 3), ("relay", 1, 0, 0), ("activate", 0, 0), ("activate", 0, 1), ("ring", 2, 0), ("relay", 1, 0, 1),
    ("gather", 2), ("project", 2, 0), ("project", 2, 1), ("ring", 3, 2), ("relay", 2, 0, 1), ("ring", 3, 1),
    ("forward", 0, 1), ("forward", 0, 0), ("ring", 3, 0), ("activate", 1, 1), ("activate", 1, 0), ("gather", 3),
    ("project", 3, 0), ("relay", 2, 1, 0), ("down", 0, 0), ("forward", 1, 1), ("relay", 2, 0, 0), ("forward", 1, 0),
    ("relay", 2, 1, 1), ("relay", 3, 0, 0), ("pair", 0, 0), ("project", 3, 1), ("down", 0, 1), ("activate", 2, 1),
    ("relay", 3, 1, 0), ("pair", 0, 1), ("activate", 2, 0), ("down", 1, 0), ("relay", 3, 0, 1), ("relay", 3, 1, 1),
    ("forward", 2, 0), ("pair", 1, 0), ("down", 1, 1), ("forward", 2, 1), ("activate", 3, 0), ("activate", 3, 1),
    ("pair", 1, 1), ("down", 2, 0), ("forward", 3, 0), ("forward", 3, 1), ("join", 1, 0), ("join", 0, 1),
    ("down", 2, 1), ("pair", 2, 0), ("down", 3, 0), ("pair", 2, 1), ("down", 3, 1), ("join", 0, 0), ("pair", 3, 1),
    ("pair", 3, 0), ("join", 1, 1), ("join", 2, 1), ("join", 2, 0), ("finish", 0), ("join", 3, 1), ("join", 3, 0),
    ("finish", 1), ("finish", 2), ("finish", 3),
)


def fused(
    x_ref, kb_ref, gain_ref, wg_hbm, wu_hbm, wd_hbm, out_ref, chk_ref,
    wg, wu, wd, xs, xbuf, xn, kw, kall, iown, iall, word, rows_scale, keep,
    pb, hold, pown, relay, from_x, from_y, sums, hbuf, qf, qb, sib, ssend, jsend, zr, zpass, cown, csend, call,
    w_sem, rx, tx_dp, tx_z, tx_s, rk, tk, ri, ti, rp, tp, rh, th, rs, ts, rz, rpass, tz, tj, rc, tc,
):
    W, m, n, R, width = xbuf.shape
    U = wg.shape[1]
    TB = m * R
    half = TB // 2
    words = kb_ref.shape[1] // m
    tile = 256 if U % 256 == 0 and width % 256 == 0 else 128
    step_cols = -(-(U // tile) // COL_PARTS) * tile
    parts = tuple((lo, min(step_cols, U - lo)) for lo in range(0, U, step_cols))
    span = width // 2
    halves = [pl.ds(h * span, span) for h in range(2)]

    i, j = lax.axis_index("dp"), lax.axis_index("tensor")
    iy, ix = i // 2, i % 2
    z, c = j // 2, j % 2
    xnb = iy * 2 + (1 - ix)
    ynb = (1 - iy) * 2 + ix
    diag = (1 - iy) * 2 + (1 - ix)
    sibling = z * 2 + (1 - c)
    mate = z + 1 - 2 * (z % 2)
    far, far_end = 2 - z // 2, 3 * (1 - z // 2)
    away = 2 * (1 - z // 2)
    inner = (z + 1) // 2 == 1
    outer = (z + 1) // 2 != 1
    order = (diag, ynb, xnb, i)
    sends, inner_sends, outer_sends = [], [], []

    def remote(src, dst, ss, rsem, to):
        return pltpu.make_async_remote_copy(
            src_ref=src, dst_ref=dst, send_sem=ss, recv_sem=rsem, device_id=to, device_id_type=MESH
        )

    def send(src, dst, ss, rsem, to):
        copy = remote(src, dst, ss, rsem, to)
        copy.start()
        sends.append(copy)

    def arrived(dst, rsem):
        remote(dst, dst, tc.at[0], rsem, (i, sibling)).wait_recv()

    loads = [pltpu.make_async_copy(s, d, w_sem.at[k]) for k, (s, d) in enumerate(((wg_hbm, wg), (wu_hbm, wu), (wd_hbm, wd)))]
    for load in loads:
        load.start()

    barrier = pltpu.get_barrier_semaphore()
    for other in (xnb, ynb, diag):
        pl.semaphore_signal(barrier, inc=1, device_id=(other, j), device_id_type=MESH)
    for step in range(1, m):
        pl.semaphore_signal(barrier, inc=1, device_id=(i, (j + step) % m), device_id_type=MESH)
    for w in range(W):
        for b in range(n):
            xs[w, b] = x_ref[w * R : (w + 1) * R, b * width : (b + 1) * width]
        xbuf[w, j, i] = xs[w, i]
    pl.semaphore_wait(barrier, 3 + m - 1)

    for w in range(W):
        for k, other in enumerate((diag, ynb, xnb)):
            send(xs.at[w, other], xbuf.at[w, j, i], tx_dp.at[w, k], rx.at[w, j, k], (other, j))

    kw[...] = jnp.zeros_like(kw)
    for t in range(m):
        kw[t, :, 0:words] = kb_ref[:, t * words : (t + 1) * words]
    rows = x_ref[...].astype(F32)
    total = jnp.sum(rows * rows, axis=1, keepdims=True)
    iown[...] = jnp.broadcast_to(lax.rsqrt(total / (x_ref.shape[1]) + 1e-05), iown.shape)
    iall[j] = iown[...]
    kall[j] = kw[j]

    def own(w):
        for k, b in enumerate((diag, ynb, xnb)):
            arrived(xbuf.at[w, j, b], rx.at[w, j, k])
        for q, to in enumerate((far, mate)):
            send(xbuf.at[w, j], xbuf.at[w, j], tx_z.at[w, q], rx.at[w, j, 3], (i, to * 2 + c))
        send(xbuf.at[w, j], xbuf.at[w, j], tx_s.at[w, 0], rx.at[w, j, 3], (i, sibling))

    def ring(w, q):
        slot = (mate, far, far_end)[q] * 2 + c
        arrived(xbuf.at[w, slot], rx.at[w, slot, 3])
        if q > 0:
            copy = remote(xbuf.at[w, slot], xbuf.at[w, slot], tx_z.at[w, q + 1], rx.at[w, slot, 3], (i, mate * 2 + c))
            pl.when(inner)(copy.start)
            inner_sends.append(copy)
        send(xbuf.at[w, slot], xbuf.at[w, slot], tx_s.at[w, q + 1], rx.at[w, slot, 3], (i, sibling))

    gain = gain_ref[...].astype(F32).reshape(1, width)

    def gather(w):
        for chip in (z, mate, far, far_end):
            slot = chip * 2 + (1 - c)
            arrived(xbuf.at[w, slot], rx.at[w, slot, 3])
        for k, b in enumerate(order):
            for t in range(m):
                xn[w, k * TB + t * R : k * TB + (t + 1) * R, :] = (xbuf[w, t, b].astype(F32) * gain).astype(BF16)

    def bits():
        for step in range(1, m):
            to = (j + step) % m
            send(kw.at[to], kall.at[j], tk.at[step - 1], rk.at[j], (i, to))
            send(iown, iall.at[j], ti.at[step - 1], ri.at[j], (i, to))

    def expand():
        for step in range(1, m):
            slot = (j + step) % m
            arrived(kall.at[slot], rk.at[slot])
            arrived(iall.at[slot], ri.at[slot])
        lanes = kall.shape[2]
        for w in range(W):
            for t in range(m):
                at = (w * m + t) * R
                word[at : at + R, :] = kall[t, w * R : (w + 1) * R, :]
                rows_scale[at : at + R, :] = iall[t, w * R : (w + 1) * R, :]
        packed = word[...]
        byte = [jnp.bitwise_and(jnp.right_shift(packed, 8 * q), 255).astype(F32).astype(BF16) for q in range(4)]

        def body(t, carry):
            unit = t * tile + lax.broadcasted_iota(jnp.int32, (lanes, tile), 1)
            where = lax.broadcasted_iota(jnp.int32, (lanes, tile), 0)
            spread = jnp.zeros((W * TB, tile), F32)
            for q in range(4):
                hit = (jnp.right_shift(unit, 3) == where * 4 + q)
                spread += jnp.dot(byte[q], jnp.where(hit, 1.0, 0.0).astype(BF16), preferred_element_type=F32)
            shift = jnp.bitwise_and(lax.broadcasted_iota(jnp.int32, (W * TB, tile), 1), 7)
            bit = jnp.bitwise_and(jnp.right_shift(spread.astype(jnp.int32), shift), 1)
            keep[:, pl.ds(pl.multiple_of(t * tile, tile), tile)] = (2 * bit).astype(F32)
            return carry

        lax.fori_loop(0, U // tile, body, 0)

    def project(w, p):
        if w == 0 and p == 0:
            loads[0].wait()
            loads[1].wait()
        lo, size = parts[p]
        at = pl.ds(lo, size)
        for g, wt in enumerate((wg, wu)):

            def body(t, carry):
                cols = pl.ds(pl.multiple_of(t * tile, tile), tile)
                part = jnp.dot(xn[w], wt[:, cols], preferred_element_type=F32)
                direct, kept = (2, 1) if g == 0 else (1, 2)
                pb[w, g, 0, :, cols] = part[0:TB].astype(BF16)
                pb[w, g, 1, :, cols] = part[direct * TB : (direct + 1) * TB].astype(BF16)
                hold[w, g, :, cols] = part[kept * TB : (kept + 1) * TB]
                pown[w, g, :, cols] = part[3 * TB : 4 * TB]
                return carry

            lax.fori_loop(lo // tile, (lo + size) // tile, body, 0)
            to, land = ((xnb, from_x), (ynb, from_y))[g]
            send(pb.at[w, g, 0, :, at], relay.at[w, g, :, at], tp.at[w, p, 3 * g], rp.at[w, p, 3 * g], (to, j))
            send(pb.at[w, g, 1, :, at], land.at[w, g, :, at], tp.at[w, p, 3 * g + 1], rp.at[w, p, 3 * g + 1], (to, j))

    def pass_on(w, p, g):
        lo, size = parts[p]
        at = pl.ds(lo, size)
        arrived(relay.at[w, g, :, at], rp.at[w, p, 3 * g])
        sums[w, g, :, at] = (hold[w, g, :, at] + relay[w, g, :, at].astype(F32)).astype(BF16)
        to, land = ((ynb, from_y), (xnb, from_x))[g]
        send(sums.at[w, g, :, at], land.at[w, g, :, at], tp.at[w, p, 3 * g + 2], rp.at[w, p, 3 * g + 2], (to, j))

    def activate(w, p):
        lo, size = parts[p]
        at = pl.ds(lo, size)
        arrived(from_x.at[w, 0, :, at], rp.at[w, p, 1])
        arrived(from_y.at[w, 1, :, at], rp.at[w, p, 4])
        arrived(from_y.at[w, 0, :, at], rp.at[w, p, 2])
        arrived(from_x.at[w, 1, :, at], rp.at[w, p, 5])
        scale = rows_scale[w * TB : (w + 1) * TB, 0:1]
        gate = (pown[w, 0, :, at] + from_x[w, 0, :, at].astype(F32) + from_y[w, 0, :, at].astype(F32)) * scale
        up = (pown[w, 1, :, at] + from_x[w, 1, :, at].astype(F32) + from_y[w, 1, :, at].astype(F32)) * scale
        hbuf[w, i, :, at] = (gate / (1.0 + jnp.exp(-gate)) * up * keep[w * TB : (w + 1) * TB, lo : lo + size]).astype(BF16)
        send(hbuf.at[w, i, :, at], hbuf.at[w, i, :, at], th.at[w, p, 0], rh.at[w, i, p], (xnb, j))
        send(hbuf.at[w, i, :, at], hbuf.at[w, i, :, at], th.at[w, p, 1], rh.at[w, i, p], (ynb, j))

    def forward(w, p):
        lo, size = parts[p]
        at = pl.ds(lo, size)
        src, to = ((xnb, ynb), (ynb, xnb))[(p + w) % 2]
        arrived(hbuf.at[w, src, :, at], rh.at[w, src, p])
        send(hbuf.at[w, src, :, at], hbuf.at[w, src, :, at], th.at[w, p, 2], rh.at[w, src, p], (to, j))

    def down(w, h):
        if w == 0 and h == 0:
            loads[2].wait()
        if h == 0:
            for p, (lo, size) in enumerate(parts):
                at = pl.ds(lo, size)
                src = (ynb, xnb)[(p + w) % 2]
                arrived(hbuf.at[w, src, :, at], rh.at[w, src, p])
                arrived(hbuf.at[w, diag, :, at], rh.at[w, diag, p])

        def body(t, carry):
            cols = pl.ds(pl.multiple_of(t * tile, tile), tile)
            part = jnp.dot(hbuf[w].reshape(n * TB, U), wd[:, cols], preferred_element_type=F32)
            for b in range(n):
                for r in range(2):
                    piece = part[b * TB + r * half : b * TB + (r + 1) * half]
                    qf[w, r, b, :, cols] = piece
                    qb[w, r, b, :, cols] = piece.astype(BF16)
            return carry

        lax.fori_loop(h * span // tile, (h + 1) * span // tile, body, 0)
        at = halves[h]
        send(qb.at[w, 1 - c, :, :, at], sib.at[w, :, :, at], ts.at[w, h], rs.at[w, h], (i, sibling))

    def pair(w, h):
        at = halves[h]
        arrived(sib.at[w, :, :, at], rs.at[w, h])
        both = qf[w, c, :, :, at] + sib[w, :, :, at].astype(F32)
        qf[w, c, :, :, at] = both
        ssend[w, :, :, at] = both.astype(BF16)
        passed = remote(
            ssend.at[w, pl.ds(away, 2), :, at], zpass.at[w, :, :, at], tj.at[w, h, 0], rpass.at[w, h], (i, mate * 2 + c)
        )
        pl.when(outer)(passed.start)
        outer_sends.append(passed)
        send(ssend.at[w, mate, :, at], zr.at[w, 0, :, at], tz.at[w, h], rz.at[w, 0, h], (i, mate * 2 + c))

    def join(w, h):
        at = halves[h]
        copies = [
            remote(
                jsend.at[w, q, :, at], zr.at[w, 1, :, at], tj.at[w, h, q], rz.at[w, 1, h], (i, (away + q) * 2 + c)
            )
            for q in range(2)
        ]

        @pl.when(inner)
        def _():
            arrived(zpass.at[w, :, :, at], rpass.at[w, h])
            for q in range(2):
                jsend[w, q, :, at] = (qf[w, c, away + q, :, at] + zpass[w, q, :, at].astype(F32)).astype(BF16)
                copies[q].start()

        inner_sends.extend(copies)

    def finish(w):
        value = qf[w, c, z]
        for slot in range(2):
            for h in range(2):
                arrived(zr.at[w, slot, :, halves[h]], rz.at[w, slot, h])
            value = value + zr[w, slot].astype(F32)
        qf[w, c, z] = value
        for q in range(half // R):
            result = (xbuf[w, (half // R) * c + q, z].astype(F32) + qf[w, c, z, q * R : (q + 1) * R, :]).astype(BF16)
            at = (q * W + w) * R
            out_ref[at : at + R, :] = result
            wide = result.astype(F32)
            cown[at : at + R, :] = jnp.broadcast_to(jnp.sum(wide * wide, axis=1, keepdims=True), (R, cown.shape[1]))

    table = {
        "own": own, "ring": ring, "gather": gather, "bits": bits, "expand": expand, "project": project, "relay": pass_on,
        "activate": activate, "forward": forward, "down": down, "pair": pair, "join": join, "finish": finish,
    }
    for name, *step in SCHEDULE:
        table[name](*step)

    csend[...] = jnp.transpose(cown[...])[0:8, :]
    for k, other in enumerate((xnb, ynb, diag)):
        send(csend, call.at[i], tc.at[k], rc.at[i], (other, j))
    check = csend[...]
    for other in (xnb, ynb, diag):
        arrived(call.at[other], rc.at[other])
        check = check + call[other]
    chk_ref[...] = check[0] / x_ref.shape[1]

    for copy in sends:
        copy.wait_send()
    for copy in inner_sends:
        pl.when(inner)(copy.wait_send)
    for copy in outer_sends:
        pl.when(outer)(copy.wait_send)


def on_plane(saved_input, keep_bits, norm_gain, gate_weight, up_weight, down_weight):
    n, m = lax.axis_size("dp"), lax.axis_size("tensor")
    rows, full = saved_input.shape
    width, U = gate_weight.shape
    W = WAVES
    R = rows // W
    TB = R * m
    half = TB // 2
    out_rows = n * rows
    lanes = -(-(keep_bits.shape[1] // m) // 128) * 128
    P2 = COL_PARTS
    dma = pltpu.SemaphoreType.DMA
    vmem = pl.BlockSpec(memory_space=pltpu.VMEM)
    hbm = pl.BlockSpec(memory_space=pl.ANY)
    V = pltpu.VMEM
    scratch = [
        V((width, U), BF16), V((width, U), BF16), V((U, width), BF16),
        V((W, n, R, width), BF16), V((W, m, n, R, width), BF16), V((W, n * TB, width), BF16),
        V((m, rows, lanes), jnp.int32), V((m, rows, lanes), jnp.int32),
        V((rows, 128), F32), V((m, rows, 128), F32), V((W * TB, lanes), jnp.int32), V((W * TB, 128), F32), V((W * TB, U), F32),
        V((W, 2, 2, TB, U), BF16), V((W, 2, TB, U), F32), V((W, 2, TB, U), F32),
        V((W, 2, TB, U), BF16), V((W, 2, TB, U), BF16), V((W, 2, TB, U), BF16), V((W, 2, TB, U), BF16),
        V((W, n, TB, U), BF16),
        V((W, 2, n, half, width), F32), V((W, 2, n, half, width), BF16),
        V((W, n, half, width), BF16), V((W, n, half, width), BF16), V((W, 2, half, width), BF16),
        V((W, 2, half, width), BF16), V((W, 2, half, width), BF16),
        V((out_rows, 128), F32), V((8, out_rows), F32), V((n, 8, out_rows), F32),
        dma((3,)), dma((W, m, 4)), dma((W, 3)), dma((W, 4)), dma((W, 4)),
        dma((m,)), dma((m - 1,)), dma((m,)), dma((m - 1,)),
        dma((W, P2, 6)), dma((W, P2, 6)), dma((W, n, P2)), dma((W, P2, 3)),
        dma((W, 2)), dma((W, 2)), dma((W, 2, 2)), dma((W, 2)), dma((W, 2)), dma((W, 2, 2)), dma((n,)), dma((3,)),
    ]
    layer_out, check = pl.pallas_call(
        fused,
        out_shape=(
            jax.ShapeDtypeStruct((out_rows, width), BF16),
            jax.ShapeDtypeStruct((out_rows,), F32),
        ),
        in_specs=[vmem, vmem, vmem, hbm, hbm, hbm],
        out_specs=(vmem, vmem),
        scratch_shapes=scratch,
        compiler_params=pltpu.CompilerParams(
            collective_id=0, has_side_effects=True, vmem_limit_bytes=60 * 1024 * 1024
        ),
    )(saved_input, keep_bits, norm_gain, gate_weight, up_weight, down_weight)
    return layer_out, check


def solution(mesh):
    placed = (
        P(("dp", "tensor"), None),
        P(("dp", "tensor"), None),
        P("dp"),
        P("dp", "tensor"),
        P("dp", "tensor"),
        P("tensor", "dp"),
    )
    plane = mesh.shape["dp"] == 4 and mesh.shape["tensor"] == 2 * mesh.shape["dp"]
    return jax.shard_map(
        on_plane if plane else on_device,
        mesh=mesh,
        in_specs=placed,
        out_specs=(P("tensor", "dp"), P("tensor")),
        check_vma=False,
    )
```

```python
import jax
import jax.numpy as jnp
from jax import lax
from jax.experimental import pallas as pl
from jax.experimental.pallas import tpu as pltpu
from jax.sharding import PartitionSpec as P

D = 8192


def on_device(saved_input, keep_bits, norm_gain, gate_weight, up_weight, down_weight):
    tensor_width = lax.axis_size("tensor")
    dp_width = lax.axis_size("dp")
    unit_words = lax.all_to_all(keep_bits, "tensor", split_axis=1, concat_axis=0, tiled=True)
    shifts = jnp.arange(32, dtype=jnp.int32)
    keep_mask = jnp.bitwise_and(jnp.right_shift(unit_words[:, :, None], shifts[None, None, :]), 1)
    keep_mask = keep_mask.reshape(unit_words.shape[0], -1)
    keep_scale = 2.0 * keep_mask.astype(jnp.float32)
    width_units = gate_weight.shape[1]
    columns = lax.all_to_all(saved_input, "dp", split_axis=1, concat_axis=0, tiled=True)
    collected = lax.all_gather(columns, "tensor", axis=0, tiled=True)
    per_device = saved_input.shape[0]
    collected = collected.reshape(tensor_width, dp_width, per_device, collected.shape[1])
    collected = collected.transpose(1, 0, 2, 3).reshape(-1, collected.shape[3])
    widened = collected.astype(jnp.float32)
    squares = lax.psum(jnp.sum(widened * widened, axis=1), "dp")
    inv_rms = lax.rsqrt(squares / D + 1e-05)
    normed = (widened * inv_rms[:, None] * norm_gain.astype(jnp.float32)[None, :]).astype(
        jnp.bfloat16
    )
    gate_part = jnp.dot(normed, gate_weight, preferred_element_type=jnp.float32)
    up_part = jnp.dot(normed, up_weight, preferred_element_type=jnp.float32)
    projected = lax.psum_scatter(
        jnp.concatenate((gate_part, up_part), axis=1).astype(jnp.bfloat16),
        "dp",
        scatter_dimension=0,
        tiled=True,
    ).astype(jnp.float32)
    gate_sum = projected[:, :width_units]
    up_sum = projected[:, width_units:]
    hidden = (jax.nn.silu(gate_sum) * up_sum * keep_scale).astype(jnp.bfloat16)
    partial_value = jnp.dot(
        lax.all_gather(hidden, "dp", axis=0, tiled=True),
        down_weight,
        preferred_element_type=jnp.float32,
    )
    mlp_sum = lax.psum_scatter(
        partial_value.astype(jnp.bfloat16), "tensor", scatter_dimension=0, tiled=True
    ).astype(jnp.float32)
    out_rows = mlp_sum.shape[0]
    first_row = lax.axis_index("tensor") * out_rows
    residual = lax.dynamic_slice_in_dim(collected, first_row, out_rows, 0)
    layer_out = (residual.astype(jnp.float32) + mlp_sum).astype(jnp.bfloat16)
    widened_out = layer_out.astype(jnp.float32)
    row_check = lax.psum(jnp.sum(widened_out * widened_out, axis=1), "dp") / D
    return (layer_out, row_check)


MESH = pl.DeviceIdType.MESH
F32 = jnp.float32
BF16 = jnp.bfloat16
COL_PARTS = (4, 2, 2, 4)
SPLIT_LAST = (False, False, False, True)
SENDS = 48


SCHEDULE = (
    ("bits",), ("expand", 0), ("own", 0), ("own", 1), ("spread", 0), ("gather", 0), ("project", 0, 1),
    ("project", 0, 2), ("project", 0, 0), ("project", 0, 3), ("ring", 1, 0), ("ring", 1, 1), ("relay", 0, 1, 1),
    ("relay", 0, 1, 0), ("gather", 1), ("relay", 0, 2, 1), ("relay", 0, 0, 0), ("spread", 1), ("relay", 0, 0, 1),
    ("relay", 0, 2, 0), ("project", 1, 1), ("activate", 0, 1), ("expand", 1), ("relay", 0, 3, 1), ("relay", 0, 3, 0),
    ("activate", 0, 2), ("activate", 0, 0), ("project", 1, 0), ("forward", 0, 0), ("relay", 1, 1, 1),
    ("activate", 0, 3), ("relay", 1, 1, 0), ("ring", 3, 1), ("ring", 3, 0), ("forward", 0, 2), ("ring", 2, 0),
    ("gather", 3), ("forward", 0, 1), ("relay", 1, 0, 0), ("project", 3, 2), ("relay", 1, 0, 1), ("project", 3, 3),
    ("ring", 2, 1), ("forward", 0, 3), ("activate", 1, 1), ("project", 3, 0), ("relay", 3, 2, 0), ("gather", 2),
    ("activate", 1, 0), ("project", 2, 0), ("forward", 1, 1), ("down", 0, 0, 0), ("forward", 1, 0), ("project", 2, 1),
    ("relay", 2, 0, 0), ("down", 0, 0, 1), ("pair", 0, 0), ("relay", 2, 0, 1), ("relay", 2, 1, 0), ("relay", 2, 1, 1),
    ("project", 3, 1), ("down", 1, 0, 0), ("relay", 3, 0, 0), ("activate", 2, 0), ("pair", 1, 0), ("relay", 3, 3, 1),
    ("down", 1, 0, 1), ("activate", 2, 1), ("pair", 0, 1), ("relay", 3, 3, 0), ("relay", 3, 1, 0), ("relay", 3, 0, 1),
    ("join", 0, 0), ("relay", 3, 1, 1), ("relay", 3, 2, 1), ("forward", 2, 0), ("forward", 2, 1), ("activate", 3, 0),
    ("join", 1, 0), ("activate", 3, 1), ("pair", 1, 1), ("activate", 3, 2), ("activate", 3, 3), ("forward", 3, 0),
    ("join", 0, 1), ("down", 2, 0, 0), ("forward", 3, 2), ("join", 1, 1), ("forward", 3, 1), ("down", 2, 0, 1),
    ("forward", 3, 3), ("pair", 2, 0), ("down", 3, 0, 0), ("down", 3, 1, 0), ("pair", 2, 1), ("down", 3, 0, 1),
    ("join", 2, 0), ("down", 3, 1, 1), ("pair", 3, 1), ("pair", 3, 0), ("join", 2, 1), ("join", 3, 1), ("join", 3, 0),
    ("finish", 0), ("finish", 1), ("finish", 3), ("finish", 2),
)


def fused(
    x_hbm, kb_hbm, gain_hbm, wg_hbm, wu_hbm, wd_hbm, out_hbm, chk_hbm,
    x_ref, kb_ref, gain_ref, wg, wu, wd, xbuf, xn, kw, kall, iown, iall, word, rows_scale, keep,
    pb, hold, pown, relay, land, sums, hbuf, qf, qb, sib, ssend, jsend, zr, zpass,
    oown, osend, cown, csend, call, cout,
    w_sem, in_sem, out_sem, tx, rx, rs_x, rz_x, rk, rp, rf, rh, rs, rz, rpass, ro, rc,
):
    m, n, R, width = xbuf.shape
    W = m // 2
    U = wg.shape[1]
    TB = 2 * R
    out_rows = out_hbm.shape[0]
    words = kb_ref.shape[1] // m
    tile = 256 if U % 256 == 0 and width % 256 == 0 else 128
    span = width // 2
    halves = [pl.ds(h * span, span) for h in range(2)]

    def cut(pieces):
        step = -(-(U // tile) // pieces) * tile
        return tuple((lo, min(step, U - lo)) for lo in range(0, U, step))

    parts = [cut(pieces) for pieces in COL_PARTS]
    base = [sum(COL_PARTS[:w]) for w in range(W)]

    i, j = lax.axis_index("dp"), lax.axis_index("tensor")
    iy, ix = i // 2, i % 2
    z, c = j // 2, j % 2
    xnb = iy * 2 + (1 - ix)
    ynb = (1 - iy) * 2 + ix
    diag = (1 - iy) * 2 + (1 - ix)
    sibling = z * 2 + (1 - c)
    mate = z + 1 - 2 * (z % 2)
    far, far_end = 2 - z // 2, 3 * (1 - z // 2)
    within = (z + 1) // 2
    inner, outer = within == 1, within != 1
    within = within % 2
    planes = (z, mate, far, far_end)
    order = (diag, ynb, xnb, i)
    pending = [None] * SENDS
    count = [0]

    def settle(at):
        if pending[at] is not None:
            when, copy = pending[at]
            if when is None:
                copy.wait_send()
            else:
                pl.when(when)(copy.wait_send)
            pending[at] = None

    def send(src, dst, rsem, to, when=None):
        at = count[0] % SENDS
        count[0] += 1
        settle(at)
        copy = pltpu.make_async_remote_copy(
            src_ref=src, dst_ref=dst, send_sem=tx.at[at], recv_sem=rsem, device_id=to, device_id_type=MESH
        )
        pending[at] = (when, copy)
        if when is None:
            copy.start()
        else:
            pl.when(when)(copy.start)

    def arrived(dst, rsem):
        pltpu.make_async_remote_copy(
            src_ref=dst, dst_ref=dst, send_sem=tx.at[0], recv_sem=rsem, device_id=(i, sibling), device_id_type=MESH
        ).wait_recv()

    fetch = [pltpu.make_async_copy(s, d, in_sem.at[k]) for k, (s, d) in enumerate(((x_hbm, x_ref), (kb_hbm, kb_ref), (gain_hbm, gain_ref)))]
    for copy in fetch:
        copy.start()
    barrier = pltpu.get_barrier_semaphore()
    for other in (xnb, ynb, diag):
        pl.semaphore_signal(barrier, inc=1, device_id=(other, j), device_id_type=MESH)
    for step in range(1, m):
        pl.semaphore_signal(barrier, inc=1, device_id=(i, (j + step) % m), device_id_type=MESH)
    loads = [pltpu.make_async_copy(s, d, w_sem.at[k]) for k, (s, d) in enumerate(((wg_hbm, wg), (wu_hbm, wu), (wd_hbm, wd)))]
    for load in loads:
        load.start()
    for copy in fetch:
        copy.wait()
    xbuf[j, i] = x_ref[:, pl.ds(pl.multiple_of(i * width, width), width)]
    kw[...] = jnp.zeros_like(kw)
    for t in range(m):
        kw[t, :, 0:words] = kb_ref[:, t * words : (t + 1) * words]
    cown[...] = jnp.zeros_like(cown)
    pl.semaphore_wait(barrier, 3 + m - 1)

    for k, other in enumerate((xnb, diag, ynb)):
        send(x_ref.at[:, pl.ds(pl.multiple_of(other * width, width), width)], xbuf.at[j, i], rx.at[(k + 1) // 2], (other, j))

    rows = x_ref[...].astype(F32)
    total = jnp.sum(rows * rows, axis=1, keepdims=True)
    iown[...] = jnp.broadcast_to(lax.rsqrt(total / (x_ref.shape[1]) + 1e-05), iown.shape)
    iall[j] = iown[...]
    kall[j] = kw[j]

    pair_at = (2 * iy, 2 * (1 - iy))

    def own(h):
        arrived(xbuf.at[j, pl.ds(pair_at[h], 1 + h)], rx.at[h])
        block = xbuf.at[j, pl.ds(pair_at[h], 2)]
        send(block, block, rs_x.at[0], (i, sibling))
        send(block, block, rz_x.at[0, h], (i, mate * 2 + c))

    def spread(h):
        block = xbuf.at[j, pl.ds(pair_at[h], 2)]
        send(block, block, rz_x.at[2, h], (i, far_end * 2 + c), outer)
        send(block, block, rz_x.at[2 - within, h], (i, far * 2 + c))

    def ring(w, h):
        block = xbuf.at[planes[w] * 2 + c, pl.ds(pair_at[h], 2)]
        arrived(block, rz_x.at[w - 1, h])
        if w == 2:
            send(block, block, rz_x.at[1, h], (i, mate * 2 + c), inner)
        send(block, block, rs_x.at[w], (i, sibling))

    gain = gain_ref[...].astype(F32).reshape(1, width)

    def gather(w):
        other, mine = planes[w] * 2 + (1 - c), planes[w] * 2
        arrived(xbuf.at[other], rs_x.at[w])
        for k, b in enumerate(order):
            for t in range(2):
                at = k * TB + t * R
                xn[w, at : at + R, :] = (xbuf[mine + t, b].astype(F32) * gain).astype(BF16)

    def bits():
        for step in range(1, m):
            to = (j + step) % m
            kind = jnp.where(to == sibling, 0, 1)
            send(kw.at[to], kall.at[j], rk.at[0, kind], (i, to))
            send(iown, iall.at[j], rk.at[1, kind], (i, to))

    def expand(rest):
        first, waves = (1, W - 1) if rest else (0, 1)
        arrived(kall.at[0 : m - 2] if rest else kall.at[0], rk.at[0, rest])
        arrived(iall.at[0 : m - 2] if rest else iall.at[0], rk.at[1, rest])
        lanes = kall.shape[2]
        for w in range(first, first + waves):
            for t in range(2):
                at = w * TB + t * R
                word[at : at + R, :] = kall[planes[w] * 2 + t]
                rows_scale[at : at + R, :] = iall[planes[w] * 2 + t]
        lo, high = first * TB, (first + waves) * TB
        packed = word[lo:high, :]
        byte = [jnp.bitwise_and(jnp.right_shift(packed, 8 * q), 255).astype(F32).astype(BF16) for q in range(4)]

        def body(t, carry):
            unit = t * tile + lax.broadcasted_iota(jnp.int32, (lanes, tile), 1)
            where = lax.broadcasted_iota(jnp.int32, (lanes, tile), 0)
            spread_out = jnp.zeros((waves * TB, tile), F32)
            for q in range(4):
                hit = (jnp.right_shift(unit, 3) == where * 4 + q)
                spread_out += jnp.dot(byte[q], jnp.where(hit, 1.0, 0.0).astype(BF16), preferred_element_type=F32)
            shift = jnp.bitwise_and(lax.broadcasted_iota(jnp.int32, (waves * TB, tile), 1), 7)
            bit = jnp.bitwise_and(jnp.right_shift(spread_out.astype(jnp.int32), shift), 1)
            keep[lo:high, pl.ds(pl.multiple_of(t * tile, tile), tile)] = (2 * bit).astype(F32)
            return carry

        lax.fori_loop(0, U // tile, body, 0)

    loaded = [False] * 3

    def ready(k):
        if not loaded[k]:
            loads[k].wait()
        loaded[k] = True

    def project(w, p):
        ready(0)
        ready(1)
        lo, size = parts[w][p]
        at = pl.ds(lo, size)
        for g, wt in enumerate((wg, wu)):

            def body(t, carry):
                cols = pl.ds(pl.multiple_of(t * tile, tile), tile)
                part = jnp.dot(xn[w], wt[:, cols], preferred_element_type=F32)
                direct, kept = (2, 1) if g == 0 else (1, 2)
                pb[w, g, 0, :, cols] = part[0:TB].astype(BF16)
                pb[w, g, 1, :, cols] = part[direct * TB : (direct + 1) * TB].astype(BF16)
                hold[w, g, :, cols] = part[kept * TB : (kept + 1) * TB]
                pown[w, g, :, cols] = part[3 * TB : 4 * TB]
                return carry

            lax.fori_loop(lo // tile, (lo + size) // tile, body, 0)
            to = (xnb, ynb)[g]
            send(pb.at[w, g, 0, :, at], relay.at[w, g, :, at], rp.at[base[w] + p, g], (to, j))
            send(pb.at[w, g, 1, :, at], land.at[w, g, :, at], rp.at[base[w] + p, 2], (to, j))

    def pass_on(w, p, g):
        lo, size = parts[w][p]
        at = pl.ds(lo, size)
        arrived(relay.at[w, g, :, at], rp.at[base[w] + p, g])
        sums[w, g, :, at] = (hold[w, g, :, at] + relay[w, g, :, at].astype(F32)).astype(BF16)
        send(sums.at[w, g, :, at], land.at[w, 2 + g, :, at], rp.at[base[w] + p, 2], ((ynb, xnb)[g], j))

    def activate(w, p):
        lo, size = parts[w][p]
        at = pl.ds(lo, size)
        arrived(land.at[w, :, :, at], rp.at[base[w] + p, 2])
        scale = rows_scale[w * TB : (w + 1) * TB, 0:1]
        gate = (pown[w, 0, :, at] + land[w, 0, :, at].astype(F32) + land[w, 2, :, at].astype(F32)) * scale
        up = (pown[w, 1, :, at] + land[w, 1, :, at].astype(F32) + land[w, 3, :, at].astype(F32)) * scale
        hbuf[w, i, :, at] = (gate / (1.0 + jnp.exp(-gate)) * up * keep[w * TB : (w + 1) * TB, lo : lo + size]).astype(BF16)
        k = len(groups(w)) - 1 if p in groups(w)[-1] else 0
        rest = rh.at[w, k]
        for q, to in enumerate((xnb, ynb)):
            sem = rf.at[base[w] + p] if q == (p + w) % 2 else rest
            send(hbuf.at[w, i, :, at], hbuf.at[w, i, :, at], sem, (to, j))

    def forward(w, p):
        lo, size = parts[w][p]
        at = pl.ds(lo, size)
        src, to = ((xnb, ynb), (ynb, xnb))[(p + w) % 2]
        arrived(hbuf.at[w, src, :, at], rf.at[base[w] + p])
        k = len(groups(w)) - 1 if p in groups(w)[-1] else 0
        send(hbuf.at[w, src, :, at], hbuf.at[w, src, :, at], rh.at[w, k], (to, j))

    def groups(w):
        count = len(parts[w])
        return (range(count - 1), (count - 1,)) if SPLIT_LAST[w] else (range(count),)

    def down(w, k, h):
        ready(2)
        group = groups(w)[k]
        final = k == len(groups(w)) - 1
        low, top = parts[w][group[0]][0], sum(parts[w][group[-1]])
        if h == 0:
            arrived(hbuf.at[w, 0:2, :, pl.ds(low, top - low)], rh.at[w, k])

        def body(t, carry):
            cols = pl.ds(pl.multiple_of(t * tile, tile), tile)
            part = jnp.dot(
                hbuf[w, :, :, low:top].reshape(n * TB, top - low), wd[low:top, cols], preferred_element_type=F32
            )
            for b in range(n):
                for r in range(2):
                    piece = part[b * TB + r * R : b * TB + (r + 1) * R]
                    if k:
                        piece = piece + qf[w, r, b, :, cols]
                    qf[w, r, b, :, cols] = piece
                    if final:
                        qb[w, r, b, :, cols] = piece.astype(BF16)
            return carry

        lax.fori_loop(h * span // tile, (h + 1) * span // tile, body, 0)
        if final:
            at = halves[h]
            send(qb.at[w, 1 - c, :, :, at], sib.at[w, :, :, at], rs.at[w, h], (i, sibling))

    def pair(w, h):
        at, plane = halves[h], planes[w]
        arrived(sib.at[w, :, :, at], rs.at[w, h])
        both = qf[w, c, :, :, at] + sib[w, :, :, at].astype(F32)
        qf[w, c, :, :, at] = both
        ssend[w, :, :, at] = both.astype(BF16)
        send(ssend.at[w, far, :, at], zpass.at[plane, :, at], rpass.at[plane, h], (i, mate * 2 + c), outer)
        send(ssend.at[w, far_end, :, at], zr.at[plane, 1 + within, :, at], rz.at[plane], (i, far_end * 2 + c))
        send(ssend.at[w, mate, :, at], zr.at[plane, 0, :, at], rz.at[plane], (i, mate * 2 + c))

    def join(w, h):
        at = halves[h]
        mine = w if w > 1 else 1 - w
        plane = planes[mine]

        @pl.when(inner)
        def _():
            arrived(zpass.at[plane, :, at], rpass.at[plane, h])
            jsend[w, :, at] = (qf[mine, c, far, :, at] + zpass[plane, :, at].astype(F32)).astype(BF16)

        send(jsend.at[w, :, at], zr.at[plane, 1, :, at], rz.at[plane], (i, far * 2 + c), inner)

    def finish(k):
        w = (2, 1 - within, within, 3)[k]
        plane = (far, mate + within * (z - mate), z + within * (mate - z), far_end)[k]
        @pl.when(outer)
        def _():
            arrived(zr.at[plane], rz.at[plane])

        @pl.when(inner)
        def _():
            arrived(zr.at[plane, 0:2], rz.at[plane])

        value = qf[w, c, z] + zr[plane, 0].astype(F32) + zr[plane, 1].astype(F32)
        qf[w, c, z] = value

        @pl.when(outer)
        def _():
            qf[w, c, z] = qf[w, c, z] + zr[plane, 2].astype(F32)

        result = (xbuf[plane * 2 + c, z].astype(F32) + qf[w, c, z]).astype(BF16)
        wide = result.astype(F32)
        row = pl.multiple_of(plane * TB + c * R, R)
        cown[pl.ds(row, R), :] = jnp.broadcast_to(jnp.sum(wide * wide, axis=1, keepdims=True), (R, cown.shape[1]))
        osend[plane] = result
        here = plane // 2 == c
        slot = plane % 2

        @pl.when(here)
        def _():
            oown[2 * slot + c] = result

        send(osend.at[plane], oown.at[2 * slot + c], ro.at[0], (i, sibling), jnp.logical_not(here))

    table = {
        "own": own, "spread": spread, "ring": ring, "gather": gather, "bits": bits, "expand": expand, "project": project, "relay": pass_on,
        "activate": activate, "forward": forward, "down": down, "pair": pair, "join": join, "finish": finish,
    }
    for name, *step in SCHEDULE:
        table[name](*step)

    csend[...] = jnp.transpose(cown[...])[0:8, :]
    for k, other in enumerate((diag, xnb, ynb)):
        for t in range(2):
            send(csend, call.at[2 * k + c], rc.at[0], (other, z * 2 + t))
    send(csend, call.at[6], rc.at[0], (i, sibling))
    arrived(oown.at[0:2], ro.at[0])
    result_out = [pltpu.make_async_copy(oown.at[q], out_hbm.at[q * R : (q + 1) * R, :], out_sem.at[q]) for q in range(4)]
    for copy in result_out:
        copy.start()
    arrived(call, rc.at[0])
    check = csend[...]
    for k in range(7):
        check = check + call[k]
    check = check / x_ref.shape[1]
    cout[...] = jnp.where(c == 0, check[0, 0:out_rows], check[0, out_rows : 2 * out_rows])
    last_copy = pltpu.make_async_copy(cout, chk_hbm, out_sem.at[4])
    last_copy.start()

    for at in range(SENDS):
        settle(at)
    for copy in result_out:
        copy.wait()
    last_copy.wait()


def on_plane(saved_input, keep_bits, norm_gain, gate_weight, up_weight, down_weight):
    n, m = lax.axis_size("dp"), lax.axis_size("tensor")
    R, full = saved_input.shape
    width, U = gate_weight.shape
    W = m // 2
    TB = 2 * R
    out_rows = n * R
    lanes = -(-(keep_bits.shape[1] // m) // 128) * 128
    P2 = sum(COL_PARTS)
    dma = pltpu.SemaphoreType.DMA
    hbm = pl.BlockSpec(memory_space=pl.ANY)
    V = pltpu.VMEM
    scratch = [
        V((R, full), BF16), V(keep_bits.shape, jnp.int32), V((width,), BF16),
        V((width, U), BF16), V((width, U), BF16), V((U, width), BF16),
        V((m, n, R, width), BF16), V((W, n * TB, width), BF16),
        V((m, R, lanes), jnp.int32), V((m, R, lanes), jnp.int32),
        V((R, 128), F32), V((m, R, 128), F32), V((W * TB, lanes), jnp.int32), V((W * TB, 128), F32), V((W * TB, U), F32),
        V((W, 2, 2, TB, U), BF16), V((W, 2, TB, U), F32), V((W, 2, TB, U), F32),
        V((W, 2, TB, U), BF16), V((W, 4, TB, U), BF16), V((W, 2, TB, U), BF16),
        V((W, n, TB, U), BF16),
        V((W, 2, n, R, width), F32), V((W, 2, n, R, width), BF16),
        V((W, n, R, width), BF16), V((W, n, R, width), BF16), V((W, R, width), BF16),
        V((W, 3, R, width), BF16), V((W, R, width), BF16),
        V((n, R, width), BF16), V((W, R, width), BF16),
        V((W * TB, 128), F32), V((8, W * TB), F32), V((7, 8, W * TB), F32), V((out_rows,), F32),
        dma((3,)), dma((3,)), dma((5,)), dma((SENDS,)), dma((2,)), dma((W,)), dma((3, 2)), dma((2, 2)),
        dma((P2, 3)), dma((P2,)), dma((W, 2)), dma((W, 2)), dma((W,)), dma((W, 2)), dma((1,)), dma((1,)),
    ]
    layer_out, check = pl.pallas_call(
        fused,
        out_shape=(
            jax.ShapeDtypeStruct((out_rows, width), BF16),
            jax.ShapeDtypeStruct((out_rows,), F32),
        ),
        in_specs=[hbm] * 6,
        out_specs=(hbm, hbm),
        scratch_shapes=scratch,
        compiler_params=pltpu.CompilerParams(
            collective_id=0, has_side_effects=True, vmem_limit_bytes=60 * 1024 * 1024
        ),
    )(saved_input, keep_bits, norm_gain, gate_weight, up_weight, down_weight)
    return layer_out, check


def solution(mesh):
    placed = (
        P(("dp", "tensor"), None),
        P(("dp", "tensor"), None),
        P("dp"),
        P("dp", "tensor"),
        P("dp", "tensor"),
        P("tensor", "dp"),
    )
    plane = mesh.shape["dp"] == 4 and mesh.shape["tensor"] == 2 * mesh.shape["dp"]
    return jax.shard_map(
        on_plane if plane else on_device,
        mesh=mesh,
        in_specs=placed,
        out_specs=(P("tensor", "dp"), P("tensor")),
        check_vma=False,
    )
```

```python
import jax
import jax.numpy as jnp
from jax import lax
from jax.experimental import pallas as pl
from jax.experimental.pallas import tpu as pltpu
from jax.sharding import PartitionSpec as P

D = 8192


def on_device(saved_input, keep_bits, norm_gain, gate_weight, up_weight, down_weight):
    tensor_width = lax.axis_size("tensor")
    dp_width = lax.axis_size("dp")
    unit_words = lax.all_to_all(keep_bits, "tensor", split_axis=1, concat_axis=0, tiled=True)
    shifts = jnp.arange(32, dtype=jnp.int32)
    keep_mask = jnp.bitwise_and(jnp.right_shift(unit_words[:, :, None], shifts[None, None, :]), 1)
    keep_mask = keep_mask.reshape(unit_words.shape[0], -1)
    keep_scale = 2.0 * keep_mask.astype(jnp.float32)
    width_units = gate_weight.shape[1]
    columns = lax.all_to_all(saved_input, "dp", split_axis=1, concat_axis=0, tiled=True)
    collected = lax.all_gather(columns, "tensor", axis=0, tiled=True)
    per_device = saved_input.shape[0]
    collected = collected.reshape(tensor_width, dp_width, per_device, collected.shape[1])
    collected = collected.transpose(1, 0, 2, 3).reshape(-1, collected.shape[3])
    widened = collected.astype(jnp.float32)
    squares = lax.psum(jnp.sum(widened * widened, axis=1), "dp")
    inv_rms = lax.rsqrt(squares / D + 1e-05)
    normed = (widened * inv_rms[:, None] * norm_gain.astype(jnp.float32)[None, :]).astype(
        jnp.bfloat16
    )
    gate_part = jnp.dot(normed, gate_weight, preferred_element_type=jnp.float32)
    up_part = jnp.dot(normed, up_weight, preferred_element_type=jnp.float32)
    projected = lax.psum_scatter(
        jnp.concatenate((gate_part, up_part), axis=1).astype(jnp.bfloat16),
        "dp",
        scatter_dimension=0,
        tiled=True,
    ).astype(jnp.float32)
    gate_sum = projected[:, :width_units]
    up_sum = projected[:, width_units:]
    hidden = (jax.nn.silu(gate_sum) * up_sum * keep_scale).astype(jnp.bfloat16)
    partial_value = jnp.dot(
        lax.all_gather(hidden, "dp", axis=0, tiled=True),
        down_weight,
        preferred_element_type=jnp.float32,
    )
    mlp_sum = lax.psum_scatter(
        partial_value.astype(jnp.bfloat16), "tensor", scatter_dimension=0, tiled=True
    ).astype(jnp.float32)
    out_rows = mlp_sum.shape[0]
    first_row = lax.axis_index("tensor") * out_rows
    residual = lax.dynamic_slice_in_dim(collected, first_row, out_rows, 0)
    layer_out = (residual.astype(jnp.float32) + mlp_sum).astype(jnp.bfloat16)
    widened_out = layer_out.astype(jnp.float32)
    row_check = lax.psum(jnp.sum(widened_out * widened_out, axis=1), "dp") / D
    return (layer_out, row_check)


MESH = pl.DeviceIdType.MESH
F32 = jnp.float32
BF16 = jnp.bfloat16
COL_PARTS = (4, 2, 2, 4)
SPLIT_LAST = (False, False, False, True)
SENDS = 48


SCHEDULE = (
    ("bits",), ("expand", 0), ("own", 0), ("own", 1), ("spread", 0), ("gather", 0), ("project", 0, 1),
    ("project", 0, 2), ("project", 0, 0), ("project", 0, 3), ("ring", 1, 0), ("ring", 1, 1), ("relay", 0, 1, 1),
    ("relay", 0, 1, 0), ("gather", 1), ("relay", 0, 2, 1), ("relay", 0, 0, 0), ("spread", 1), ("relay", 0, 0, 1),
    ("relay", 0, 2, 0), ("project", 1, 1), ("activate", 0, 1), ("expand", 1), ("relay", 0, 3, 1), ("relay", 0, 3, 0),
    ("activate", 0, 2), ("activate", 0, 0), ("project", 1, 0), ("forward", 0, 0), ("relay", 1, 1, 1),
    ("activate", 0, 3), ("relay", 1, 1, 0), ("ring", 3, 1), ("ring", 3, 0), ("forward", 0, 2), ("ring", 2, 0),
    ("gather", 3), ("forward", 0, 1), ("relay", 1, 0, 0), ("project", 3, 2), ("relay", 1, 0, 1), ("project", 3, 3),
    ("ring", 2, 1), ("forward", 0, 3), ("activate", 1, 1), ("project", 3, 0), ("relay", 3, 2, 0), ("gather", 2),
    ("activate", 1, 0), ("project", 2, 0), ("forward", 1, 1), ("down", 0, 0, 0), ("forward", 1, 0), ("project", 2, 1),
    ("relay", 2, 0, 0), ("down", 0, 0, 1), ("pair", 0, 0), ("relay", 2, 0, 1), ("relay", 2, 1, 0), ("relay", 2, 1, 1),
    ("project", 3, 1), ("down", 1, 0, 0), ("relay", 3, 0, 0), ("activate", 2, 0), ("pair", 1, 0), ("relay", 3, 3, 1),
    ("down", 1, 0, 1), ("activate", 2, 1), ("pair", 0, 1), ("relay", 3, 3, 0), ("relay", 3, 1, 0), ("relay", 3, 0, 1),
    ("join", 0, 0), ("relay", 3, 1, 1), ("relay", 3, 2, 1), ("forward", 2, 0), ("forward", 2, 1), ("activate", 3, 0),
    ("join", 1, 0), ("activate", 3, 1), ("pair", 1, 1), ("activate", 3, 2), ("activate", 3, 3), ("forward", 3, 0),
    ("join", 0, 1), ("down", 2, 0, 0), ("forward", 3, 2), ("join", 1, 1), ("forward", 3, 1), ("down", 2, 0, 1),
    ("forward", 3, 3), ("pair", 2, 0), ("down", 3, 0, 0), ("down", 3, 1, 0), ("pair", 2, 1), ("down", 3, 0, 1),
    ("join", 2, 0), ("down", 3, 1, 1), ("pair", 3, 1), ("pair", 3, 0), ("join", 2, 1), ("join", 3, 1), ("join", 3, 0),
    ("finish", 0), ("finish", 1), ("finish", 3), ("finish", 2),
)


def fused(
    x_hbm, kb_hbm, gain_hbm, wg_hbm, wu_hbm, wd_hbm, out_ref, chk_ref,
    x_ref, kb_ref, gain_ref, wg, wu, wd, xbuf, xn, kw, kall, iown, iall, word, rows_scale, keep,
    pb, hold, pown, relay, land, sums, hbuf, qf, qb, sib, ssend, jsend, zr, zpass,
    oown, osend, cown, csend, call,
    w_sem, in_sem, tx, rx, rs_x, rz_x, rk, rp, rf, rh, rs, rz, rpass, ro, rc,
):
    m, n, R, width = xbuf.shape
    W = m // 2
    U = wg.shape[1]
    TB = 2 * R
    out_rows = out_ref.shape[0]
    words = kb_ref.shape[1] // m
    tile = 256 if U % 256 == 0 and width % 256 == 0 else 128
    span = width // 2
    halves = [pl.ds(h * span, span) for h in range(2)]

    def cut(pieces):
        step = -(-(U // tile) // pieces) * tile
        return tuple((lo, min(step, U - lo)) for lo in range(0, U, step))

    parts = [cut(pieces) for pieces in COL_PARTS]
    base = [sum(COL_PARTS[:w]) for w in range(W)]

    i, j = lax.axis_index("dp"), lax.axis_index("tensor")
    iy, ix = i // 2, i % 2
    z, c = j // 2, j % 2
    xnb = iy * 2 + (1 - ix)
    ynb = (1 - iy) * 2 + ix
    diag = (1 - iy) * 2 + (1 - ix)
    sibling = z * 2 + (1 - c)
    mate = z + 1 - 2 * (z % 2)
    far, far_end = 2 - z // 2, 3 * (1 - z // 2)
    within = (z + 1) // 2
    inner, outer = within == 1, within != 1
    within = within % 2
    planes = (z, mate, far, far_end)
    order = (diag, ynb, xnb, i)
    pending = [None] * SENDS
    count = [0]

    def settle(at):
        if pending[at] is not None:
            when, copy = pending[at]
            if when is None:
                copy.wait_send()
            else:
                pl.when(when)(copy.wait_send)
            pending[at] = None

    def send(src, dst, rsem, to, when=None):
        at = count[0] % SENDS
        count[0] += 1
        settle(at)
        copy = pltpu.make_async_remote_copy(
            src_ref=src, dst_ref=dst, send_sem=tx.at[at], recv_sem=rsem, device_id=to, device_id_type=MESH
        )
        pending[at] = (when, copy)
        if when is None:
            copy.start()
        else:
            pl.when(when)(copy.start)

    def arrived(dst, rsem):
        pltpu.make_async_remote_copy(
            src_ref=dst, dst_ref=dst, send_sem=tx.at[0], recv_sem=rsem, device_id=(i, sibling), device_id_type=MESH
        ).wait_recv()

    fetch = [pltpu.make_async_copy(s, d, in_sem.at[k]) for k, (s, d) in enumerate(((x_hbm, x_ref), (kb_hbm, kb_ref), (gain_hbm, gain_ref)))]
    for copy in fetch:
        copy.start()
    barrier = pltpu.get_barrier_semaphore()
    for other in (xnb, ynb, diag):
        pl.semaphore_signal(barrier, inc=1, device_id=(other, j), device_id_type=MESH)
    for step in range(1, m):
        pl.semaphore_signal(barrier, inc=1, device_id=(i, (j + step) % m), device_id_type=MESH)
    loads = [pltpu.make_async_copy(s, d, w_sem.at[k]) for k, (s, d) in enumerate(((wg_hbm, wg), (wu_hbm, wu), (wd_hbm, wd)))]
    for load in loads:
        load.start()
    for copy in fetch:
        copy.wait()
    xbuf[j, i] = x_ref[:, pl.ds(pl.multiple_of(i * width, width), width)]
    kw[...] = jnp.zeros_like(kw)
    for t in range(m):
        kw[t, :, 0:words] = kb_ref[:, t * words : (t + 1) * words]
    cown[...] = jnp.zeros_like(cown)
    pl.semaphore_wait(barrier, 3 + m - 1)

    for k, other in enumerate((xnb, diag, ynb)):
        send(x_ref.at[:, pl.ds(pl.multiple_of(other * width, width), width)], xbuf.at[j, i], rx.at[(k + 1) // 2], (other, j))

    rows = x_ref[...].astype(F32)
    total = jnp.sum(rows * rows, axis=1, keepdims=True)
    iown[...] = jnp.broadcast_to(lax.rsqrt(total / (x_ref.shape[1]) + 1e-05), iown.shape)
    iall[j] = iown[...]
    kall[j] = kw[j]

    pair_at = (2 * iy, 2 * (1 - iy))

    def own(h):
        arrived(xbuf.at[j, pl.ds(pair_at[h], 1 + h)], rx.at[h])
        block = xbuf.at[j, pl.ds(pair_at[h], 2)]
        send(block, block, rs_x.at[0], (i, sibling))
        send(block, block, rz_x.at[0, h], (i, mate * 2 + c))

    def spread(h):
        block = xbuf.at[j, pl.ds(pair_at[h], 2)]
        send(block, block, rz_x.at[2, h], (i, far_end * 2 + c), outer)
        send(block, block, rz_x.at[2 - within, h], (i, far * 2 + c))

    def ring(w, h):
        block = xbuf.at[planes[w] * 2 + c, pl.ds(pair_at[h], 2)]
        arrived(block, rz_x.at[w - 1, h])
        if w == 2:
            send(block, block, rz_x.at[1, h], (i, mate * 2 + c), inner)
        send(block, block, rs_x.at[w], (i, sibling))

    gain = gain_ref[...].astype(F32).reshape(1, width)

    def gather(w):
        other, mine = planes[w] * 2 + (1 - c), planes[w] * 2
        arrived(xbuf.at[other], rs_x.at[w])
        for k, b in enumerate(order):
            for t in range(2):
                at = k * TB + t * R
                xn[w, at : at + R, :] = (xbuf[mine + t, b].astype(F32) * gain).astype(BF16)

    def bits():
        for step in range(1, m):
            to = (j + step) % m
            kind = jnp.where(to == sibling, 0, 1)
            send(kw.at[to], kall.at[j], rk.at[0, kind], (i, to))
            send(iown, iall.at[j], rk.at[1, kind], (i, to))

    def expand(rest):
        first, waves = (1, W - 1) if rest else (0, 1)
        arrived(kall.at[0 : m - 2] if rest else kall.at[0], rk.at[0, rest])
        arrived(iall.at[0 : m - 2] if rest else iall.at[0], rk.at[1, rest])
        lanes = kall.shape[2]
        for w in range(first, first + waves):
            for t in range(2):
                at = w * TB + t * R
                word[at : at + R, :] = kall[planes[w] * 2 + t]
                rows_scale[at : at + R, :] = iall[planes[w] * 2 + t]
        lo, high = first * TB, (first + waves) * TB
        packed = word[lo:high, :]
        byte = [jnp.bitwise_and(jnp.right_shift(packed, 8 * q), 255).astype(F32).astype(BF16) for q in range(4)]

        def body(t, carry):
            unit = t * tile + lax.broadcasted_iota(jnp.int32, (lanes, tile), 1)
            where = lax.broadcasted_iota(jnp.int32, (lanes, tile), 0)
            spread_out = jnp.zeros((waves * TB, tile), F32)
            for q in range(4):
                hit = (jnp.right_shift(unit, 3) == where * 4 + q)
                spread_out += jnp.dot(byte[q], jnp.where(hit, 1.0, 0.0).astype(BF16), preferred_element_type=F32)
            shift = jnp.bitwise_and(lax.broadcasted_iota(jnp.int32, (waves * TB, tile), 1), 7)
            bit = jnp.bitwise_and(jnp.right_shift(spread_out.astype(jnp.int32), shift), 1)
            keep[lo:high, pl.ds(pl.multiple_of(t * tile, tile), tile)] = (2 * bit).astype(F32)
            return carry

        lax.fori_loop(0, U // tile, body, 0)

    loaded = [False] * 3

    def ready(k):
        if not loaded[k]:
            loads[k].wait()
        loaded[k] = True

    def project(w, p):
        ready(0)
        ready(1)
        lo, size = parts[w][p]
        at = pl.ds(lo, size)
        for g, wt in enumerate((wg, wu)):

            def body(t, carry):
                cols = pl.ds(pl.multiple_of(t * tile, tile), tile)
                part = jnp.dot(xn[w], wt[:, cols], preferred_element_type=F32)
                direct, kept = (2, 1) if g == 0 else (1, 2)
                pb[w, g, 0, :, cols] = part[0:TB].astype(BF16)
                pb[w, g, 1, :, cols] = part[direct * TB : (direct + 1) * TB].astype(BF16)
                hold[w, g, :, cols] = part[kept * TB : (kept + 1) * TB]
                pown[w, g, :, cols] = part[3 * TB : 4 * TB]
                return carry

            lax.fori_loop(lo // tile, (lo + size) // tile, body, 0)
            to = (xnb, ynb)[g]
            send(pb.at[w, g, 0, :, at], relay.at[w, g, :, at], rp.at[base[w] + p, g], (to, j))
            send(pb.at[w, g, 1, :, at], land.at[w, g, :, at], rp.at[base[w] + p, 2], (to, j))

    def pass_on(w, p, g):
        lo, size = parts[w][p]
        at = pl.ds(lo, size)
        arrived(relay.at[w, g, :, at], rp.at[base[w] + p, g])
        sums[w, g, :, at] = (hold[w, g, :, at] + relay[w, g, :, at].astype(F32)).astype(BF16)
        send(sums.at[w, g, :, at], land.at[w, 2 + g, :, at], rp.at[base[w] + p, 2], ((ynb, xnb)[g], j))

    def activate(w, p):
        lo, size = parts[w][p]
        at = pl.ds(lo, size)
        arrived(land.at[w, :, :, at], rp.at[base[w] + p, 2])
        scale = rows_scale[w * TB : (w + 1) * TB, 0:1]
        gate = (pown[w, 0, :, at] + land[w, 0, :, at].astype(F32) + land[w, 2, :, at].astype(F32)) * scale
        up = (pown[w, 1, :, at] + land[w, 1, :, at].astype(F32) + land[w, 3, :, at].astype(F32)) * scale
        hbuf[w, i, :, at] = (gate / (1.0 + jnp.exp(-gate)) * up * keep[w * TB : (w + 1) * TB, lo : lo + size]).astype(BF16)
        k = len(groups(w)) - 1 if p in groups(w)[-1] else 0
        rest = rh.at[w, k]
        for q, to in enumerate((xnb, ynb)):
            sem = rf.at[base[w] + p] if q == (p + w) % 2 else rest
            send(hbuf.at[w, i, :, at], hbuf.at[w, i, :, at], sem, (to, j))

    def forward(w, p):
        lo, size = parts[w][p]
        at = pl.ds(lo, size)
        src, to = ((xnb, ynb), (ynb, xnb))[(p + w) % 2]
        arrived(hbuf.at[w, src, :, at], rf.at[base[w] + p])
        k = len(groups(w)) - 1 if p in groups(w)[-1] else 0
        send(hbuf.at[w, src, :, at], hbuf.at[w, src, :, at], rh.at[w, k], (to, j))

    def groups(w):
        count = len(parts[w])
        return (range(count - 1), (count - 1,)) if SPLIT_LAST[w] else (range(count),)

    def down(w, k, h):
        ready(2)
        group = groups(w)[k]
        final = k == len(groups(w)) - 1
        low, top = parts[w][group[0]][0], sum(parts[w][group[-1]])
        if h == 0:
            arrived(hbuf.at[w, 0:2, :, pl.ds(low, top - low)], rh.at[w, k])

        def body(t, carry):
            cols = pl.ds(pl.multiple_of(t * tile, tile), tile)
            part = jnp.dot(
                hbuf[w, :, :, low:top].reshape(n * TB, top - low), wd[low:top, cols], preferred_element_type=F32
            )
            for b in range(n):
                for r in range(2):
                    piece = part[b * TB + r * R : b * TB + (r + 1) * R]
                    if k:
                        piece = piece + qf[w, r, b, :, cols]
                    qf[w, r, b, :, cols] = piece
                    if final:
                        qb[w, r, b, :, cols] = piece.astype(BF16)
            return carry

        lax.fori_loop(h * span // tile, (h + 1) * span // tile, body, 0, unroll=True)
        if final:
            at = halves[h]
            send(qb.at[w, 1 - c, :, :, at], sib.at[w, :, :, at], rs.at[w, h], (i, sibling))

    def pair(w, h):
        at, plane = halves[h], planes[w]
        arrived(sib.at[w, :, :, at], rs.at[w, h])
        both = qf[w, c, :, :, at] + sib[w, :, :, at].astype(F32)
        qf[w, c, :, :, at] = both
        ssend[w, :, :, at] = both.astype(BF16)
        send(ssend.at[w, far, :, at], zpass.at[plane, :, at], rpass.at[plane, h], (i, mate * 2 + c), outer)
        send(ssend.at[w, far_end, :, at], zr.at[plane, 1 + within, :, at], rz.at[plane], (i, far_end * 2 + c))
        send(ssend.at[w, mate, :, at], zr.at[plane, 0, :, at], rz.at[plane], (i, mate * 2 + c))

    def join(w, h):
        at = halves[h]
        mine = w if w > 1 else 1 - w
        plane = planes[mine]

        @pl.when(inner)
        def _():
            arrived(zpass.at[plane, :, at], rpass.at[plane, h])
            jsend[w, :, at] = (qf[mine, c, far, :, at] + zpass[plane, :, at].astype(F32)).astype(BF16)

        send(jsend.at[w, :, at], zr.at[plane, 1, :, at], rz.at[plane], (i, far * 2 + c), inner)

    def finish(k):
        w = (2, 1 - within, within, 3)[k]
        plane = (far, mate + within * (z - mate), z + within * (mate - z), far_end)[k]
        @pl.when(outer)
        def _():
            arrived(zr.at[plane], rz.at[plane])

        @pl.when(inner)
        def _():
            arrived(zr.at[plane, 0:2], rz.at[plane])

        value = qf[w, c, z] + zr[plane, 0].astype(F32) + zr[plane, 1].astype(F32)
        qf[w, c, z] = value

        @pl.when(outer)
        def _():
            qf[w, c, z] = qf[w, c, z] + zr[plane, 2].astype(F32)

        result = (xbuf[plane * 2 + c, z].astype(F32) + qf[w, c, z]).astype(BF16)
        wide = result.astype(F32)
        row = pl.multiple_of(plane * TB + c * R, R)
        cown[pl.ds(row, R), :] = jnp.broadcast_to(jnp.sum(wide * wide, axis=1, keepdims=True), (R, cown.shape[1]))
        osend[plane] = result
        here = plane // 2 == c
        slot = plane % 2

        @pl.when(here)
        def _():
            oown[2 * slot + c] = result

        send(osend.at[plane], oown.at[2 * slot + c], ro.at[0], (i, sibling), jnp.logical_not(here))

    table = {
        "own": own, "spread": spread, "ring": ring, "gather": gather, "bits": bits, "expand": expand, "project": project, "relay": pass_on,
        "activate": activate, "forward": forward, "down": down, "pair": pair, "join": join, "finish": finish,
    }
    for name, *step in SCHEDULE:
        table[name](*step)

    csend[...] = jnp.transpose(cown[...])[0:8, :]
    for k, other in enumerate((diag, xnb, ynb)):
        for t in range(2):
            send(csend, call.at[2 * k + c], rc.at[0], (other, z * 2 + t))
    send(csend, call.at[6], rc.at[0], (i, sibling))
    arrived(oown.at[0:2], ro.at[0])
    for q in range(4):
        out_ref[q * R : (q + 1) * R, :] = oown[q]
    arrived(call, rc.at[0])
    check = csend[...]
    for k in range(7):
        check = check + call[k]
    check = check / x_ref.shape[1]
    chk_ref[...] = jnp.where(c == 0, check[0, 0:out_rows], check[0, out_rows : 2 * out_rows])

    for at in range(SENDS):
        settle(at)


def on_plane(saved_input, keep_bits, norm_gain, gate_weight, up_weight, down_weight):
    n, m = lax.axis_size("dp"), lax.axis_size("tensor")
    R, full = saved_input.shape
    width, U = gate_weight.shape
    W = m // 2
    TB = 2 * R
    out_rows = n * R
    lanes = -(-(keep_bits.shape[1] // m) // 128) * 128
    P2 = sum(COL_PARTS)
    dma = pltpu.SemaphoreType.DMA
    vmem = pl.BlockSpec(memory_space=pltpu.VMEM)
    hbm = pl.BlockSpec(memory_space=pl.ANY)
    V = pltpu.VMEM
    scratch = [
        V((R, full), BF16), V(keep_bits.shape, jnp.int32), V((width,), BF16),
        V((width, U), BF16), V((width, U), BF16), V((U, width), BF16),
        V((m, n, R, width), BF16), V((W, n * TB, width), BF16),
        V((m, R, lanes), jnp.int32), V((m, R, lanes), jnp.int32),
        V((R, 128), F32), V((m, R, 128), F32), V((W * TB, lanes), jnp.int32), V((W * TB, 128), F32), V((W * TB, U), F32),
        V((W, 2, 2, TB, U), BF16), V((W, 2, TB, U), F32), V((W, 2, TB, U), F32),
        V((W, 2, TB, U), BF16), V((W, 4, TB, U), BF16), V((W, 2, TB, U), BF16),
        V((W, n, TB, U), BF16),
        V((W, 2, n, R, width), F32), V((W, 2, n, R, width), BF16),
        V((W, n, R, width), BF16), V((W, n, R, width), BF16), V((W, R, width), BF16),
        V((W, 3, R, width), BF16), V((W, R, width), BF16),
        V((n, R, width), BF16), V((W, R, width), BF16),
        V((W * TB, 128), F32), V((8, W * TB), F32), V((7, 8, W * TB), F32),
        dma((3,)), dma((3,)), dma((SENDS,)), dma((2,)), dma((W,)), dma((3, 2)), dma((2, 2)),
        dma((P2, 3)), dma((P2,)), dma((W, 2)), dma((W, 2)), dma((W,)), dma((W, 2)), dma((1,)), dma((1,)),
    ]
    layer_out, check = pl.pallas_call(
        fused,
        out_shape=(
            pltpu.VMEM((out_rows, width), BF16),
            pltpu.VMEM((out_rows,), F32),
        ),
        in_specs=[hbm] * 6,
        out_specs=(vmem, vmem),
        scratch_shapes=scratch,
        compiler_params=pltpu.CompilerParams(
            collective_id=0, has_side_effects=True, vmem_limit_bytes=60 * 1024 * 1024
        ),
    )(saved_input, keep_bits, norm_gain, gate_weight, up_weight, down_weight)
    return layer_out, check


def solution(mesh):
    placed = (
        P(("dp", "tensor"), None),
        P(("dp", "tensor"), None),
        P("dp"),
        P("dp", "tensor"),
        P("dp", "tensor"),
        P("tensor", "dp"),
    )
    plane = mesh.shape["dp"] == 4 and mesh.shape["tensor"] == 2 * mesh.shape["dp"]
    return jax.shard_map(
        on_plane if plane else on_device,
        mesh=mesh,
        in_specs=placed,
        out_specs=(P("tensor", "dp"), P("tensor")),
        check_vma=False,
    )
```

```python
import jax
import jax.numpy as jnp
from jax import lax
from jax.experimental import pallas as pl
from jax.experimental.pallas import tpu as pltpu
from jax.sharding import PartitionSpec as P

D = 8192


def on_device(saved_input, keep_bits, norm_gain, gate_weight, up_weight, down_weight):
    tensor_width = lax.axis_size("tensor")
    dp_width = lax.axis_size("dp")
    unit_words = lax.all_to_all(keep_bits, "tensor", split_axis=1, concat_axis=0, tiled=True)
    shifts = jnp.arange(32, dtype=jnp.int32)
    keep_mask = jnp.bitwise_and(jnp.right_shift(unit_words[:, :, None], shifts[None, None, :]), 1)
    keep_mask = keep_mask.reshape(unit_words.shape[0], -1)
    keep_scale = 2.0 * keep_mask.astype(jnp.float32)
    width_units = gate_weight.shape[1]
    columns = lax.all_to_all(saved_input, "dp", split_axis=1, concat_axis=0, tiled=True)
    collected = lax.all_gather(columns, "tensor", axis=0, tiled=True)
    per_device = saved_input.shape[0]
    collected = collected.reshape(tensor_width, dp_width, per_device, collected.shape[1])
    collected = collected.transpose(1, 0, 2, 3).reshape(-1, collected.shape[3])
    widened = collected.astype(jnp.float32)
    squares = lax.psum(jnp.sum(widened * widened, axis=1), "dp")
    inv_rms = lax.rsqrt(squares / D + 1e-05)
    normed = (widened * inv_rms[:, None] * norm_gain.astype(jnp.float32)[None, :]).astype(
        jnp.bfloat16
    )
    gate_part = jnp.dot(normed, gate_weight, preferred_element_type=jnp.float32)
    up_part = jnp.dot(normed, up_weight, preferred_element_type=jnp.float32)
    projected = lax.psum_scatter(
        jnp.concatenate((gate_part, up_part), axis=1).astype(jnp.bfloat16),
        "dp",
        scatter_dimension=0,
        tiled=True,
    ).astype(jnp.float32)
    gate_sum = projected[:, :width_units]
    up_sum = projected[:, width_units:]
    hidden = (jax.nn.silu(gate_sum) * up_sum * keep_scale).astype(jnp.bfloat16)
    partial_value = jnp.dot(
        lax.all_gather(hidden, "dp", axis=0, tiled=True),
        down_weight,
        preferred_element_type=jnp.float32,
    )
    mlp_sum = lax.psum_scatter(
        partial_value.astype(jnp.bfloat16), "tensor", scatter_dimension=0, tiled=True
    ).astype(jnp.float32)
    out_rows = mlp_sum.shape[0]
    first_row = lax.axis_index("tensor") * out_rows
    residual = lax.dynamic_slice_in_dim(collected, first_row, out_rows, 0)
    layer_out = (residual.astype(jnp.float32) + mlp_sum).astype(jnp.bfloat16)
    widened_out = layer_out.astype(jnp.float32)
    row_check = lax.psum(jnp.sum(widened_out * widened_out, axis=1), "dp") / D
    return (layer_out, row_check)


MESH = pl.DeviceIdType.MESH
F32 = jnp.float32
BF16 = jnp.bfloat16
COL_PARTS = (4, 2, 2, 4)
SPLIT_LAST = (False, False, False, True)
SENDS = 48


SCHEDULE = (
    ("bits",), ("own", 0), ("own", 1), ("spread", 0), ("gather", 0), ("spread", 1), ("project", 0, 0),
    ("project", 0, 1), ("project", 0, 2), ("project", 0, 3), ("relay", 0, 0, 1), ("relay", 0, 1, 0), ("ring", 1, 0),
    ("ring", 1, 1), ("expand", 0), ("relay", 0, 2, 0), ("gather", 1), ("relay", 0, 1, 1), ("relay", 0, 0, 0),
    ("project", 1, 1), ("project", 1, 0), ("relay", 0, 2, 1), ("relay", 1, 1, 0), ("relay", 1, 1, 1), ("ring", 2, 0),
    ("relay", 1, 0, 1), ("relay", 1, 0, 0), ("activate", 0, 1), ("ring", 3, 0), ("relay", 0, 3, 0),
    ("relay", 0, 3, 1), ("expand", 1), ("activate", 0, 0), ("activate", 0, 2), ("ring", 3, 1), ("activate", 1, 1),
    ("ring", 2, 1), ("gather", 3), ("activate", 1, 0), ("project", 3, 3), ("activate", 0, 3), ("forward", 1, 1),
    ("forward", 0, 2), ("forward", 0, 1), ("project", 3, 2), ("gather", 2), ("project", 2, 1), ("forward", 1, 0),
    ("project", 2, 0), ("relay", 2, 1, 0), ("relay", 2, 1, 1), ("project", 3, 1), ("relay", 2, 0, 0),
    ("relay", 2, 0, 1), ("project", 3, 0), ("down", 1, 0, 0), ("down", 1, 0, 1), ("pair", 1, 1), ("forward", 0, 3),
    ("relay", 3, 1, 0), ("relay", 3, 1, 1), ("forward", 0, 0), ("relay", 3, 3, 0), ("activate", 2, 1),
    ("relay", 3, 2, 0), ("relay", 3, 2, 1), ("activate", 2, 0), ("relay", 3, 0, 1), ("down", 0, 0, 0),
    ("relay", 3, 0, 0), ("pair", 1, 0), ("forward", 2, 1), ("activate", 3, 2), ("forward", 2, 0), ("pair", 0, 0),
    ("relay", 3, 3, 1), ("down", 0, 0, 1), ("activate", 3, 0), ("activate", 3, 1), ("pair", 0, 1), ("activate", 3, 3),
    ("join", 1, 0), ("forward", 3, 2), ("down", 2, 0, 0), ("forward", 3, 1), ("forward", 3, 0), ("join", 0, 0),
    ("down", 2, 0, 1), ("join", 0, 1), ("pair", 2, 0), ("join", 1, 1), ("forward", 3, 3), ("down", 3, 0, 0),
    ("pair", 2, 1), ("down", 3, 0, 1), ("join", 2, 0), ("down", 3, 1, 0), ("down", 3, 1, 1), ("pair", 3, 1),
    ("pair", 3, 0), ("join", 2, 1), ("finish", 0), ("join", 3, 1), ("join", 3, 0), ("finish", 1), ("finish", 3),
    ("finish", 2),
)


def fused(
    x_hbm, kb_hbm, gain_hbm, wg_hbm, wu_hbm, wd_hbm, out_ref, chk_ref,
    x_ref, kb_ref, gain_ref, wg, wu, wd, xbuf, xn, kw, kall, iown, iall, word, rows_scale, keep,
    pb, hold, pown, relay, land, sums, hbuf, qf, qb, sib, ssend, jsend, zr, zpass,
    oown, osend, cown, csend, call,
    w_sem, in_sem, tx, rx, rs_x, rz_x, rk, rp, rf, rh, rs, rz, rpass, ro, rc,
):
    m, n, R, width = xbuf.shape
    W = m // 2
    U = wg.shape[1]
    TB = 2 * R
    out_rows = out_ref.shape[0]
    words = kb_ref.shape[1] // m
    tile = 256 if U % 256 == 0 and width % 256 == 0 else 128
    span = width // 2
    halves = [pl.ds(h * span, span) for h in range(2)]

    def cut(pieces):
        step = -(-(U // tile) // pieces) * tile
        return tuple((lo, min(step, U - lo)) for lo in range(0, U, step))

    parts = [cut(pieces) for pieces in COL_PARTS]
    base = [sum(COL_PARTS[:w]) for w in range(W)]

    i, j = lax.axis_index("dp"), lax.axis_index("tensor")
    iy, ix = i // 2, i % 2
    z, c = j // 2, j % 2
    xnb = iy * 2 + (1 - ix)
    ynb = (1 - iy) * 2 + ix
    diag = (1 - iy) * 2 + (1 - ix)
    sibling = z * 2 + (1 - c)
    mate = z + 1 - 2 * (z % 2)
    far, far_end = 2 - z // 2, 3 * (1 - z // 2)
    within = (z + 1) // 2
    inner, outer = within == 1, within != 1
    within = within % 2
    planes = (z, mate, far, far_end)
    order = (diag, ynb, xnb, i)
    pending = [None] * SENDS
    count = [0]

    def settle(at):
        if pending[at] is not None:
            when, copy = pending[at]
            if when is None:
                copy.wait_send()
            else:
                pl.when(when)(copy.wait_send)
            pending[at] = None

    def send(src, dst, rsem, to, when=None):
        at = count[0] % SENDS
        count[0] += 1
        settle(at)
        copy = pltpu.make_async_remote_copy(
            src_ref=src, dst_ref=dst, send_sem=tx.at[at], recv_sem=rsem, device_id=to, device_id_type=MESH
        )
        pending[at] = (when, copy)
        if when is None:
            copy.start()
        else:
            pl.when(when)(copy.start)

    def arrived(dst, rsem):
        pltpu.make_async_remote_copy(
            src_ref=dst, dst_ref=dst, send_sem=tx.at[0], recv_sem=rsem, device_id=(i, sibling), device_id_type=MESH
        ).wait_recv()

    fetch = [pltpu.make_async_copy(s, d, in_sem.at[k]) for k, (s, d) in enumerate(((x_hbm, x_ref), (kb_hbm, kb_ref), (gain_hbm, gain_ref)))]
    for copy in fetch:
        copy.start()
    barrier = pltpu.get_barrier_semaphore()
    for other in (xnb, ynb, diag):
        pl.semaphore_signal(barrier, inc=1, device_id=(other, j), device_id_type=MESH)
    for step in range(1, m):
        pl.semaphore_signal(barrier, inc=1, device_id=(i, (j + step) % m), device_id_type=MESH)
    loads = [pltpu.make_async_copy(s, d, w_sem.at[k]) for k, (s, d) in enumerate(((wg_hbm, wg), (wu_hbm, wu), (wd_hbm, wd)))]
    for load in loads:
        load.start()
    for copy in fetch:
        copy.wait()
    xbuf[j, i] = x_ref[:, pl.ds(pl.multiple_of(i * width, width), width)]
    kw[...] = jnp.zeros_like(kw)
    for t in range(m):
        kw[t, :, 0:words] = kb_ref[:, t * words : (t + 1) * words]
    cown[...] = jnp.zeros_like(cown)
    pl.semaphore_wait(barrier, 3 + m - 1)

    for k, other in enumerate((xnb, diag, ynb)):
        send(x_ref.at[:, pl.ds(pl.multiple_of(other * width, width), width)], xbuf.at[j, i], rx.at[(k + 1) // 2], (other, j))

    rows = x_ref[...].astype(F32)
    total = jnp.sum(rows * rows, axis=1, keepdims=True)
    iown[...] = jnp.broadcast_to(lax.rsqrt(total / (x_ref.shape[1]) + 1e-05), iown.shape)
    iall[j] = iown[...]
    kall[j] = kw[j]

    pair_at = (2 * iy, 2 * (1 - iy))

    def own(h):
        arrived(xbuf.at[j, pl.ds(pair_at[h], 1 + h)], rx.at[h])
        block = xbuf.at[j, pl.ds(pair_at[h], 2)]
        send(block, block, rs_x.at[0], (i, sibling))
        send(block, block, rz_x.at[0, h], (i, mate * 2 + c))

    def spread(h):
        block = xbuf.at[j, pl.ds(pair_at[h], 2)]
        send(block, block, rz_x.at[2, h], (i, far_end * 2 + c), outer)
        send(block, block, rz_x.at[2 - within, h], (i, far * 2 + c))

    def ring(w, h):
        block = xbuf.at[planes[w] * 2 + c, pl.ds(pair_at[h], 2)]
        arrived(block, rz_x.at[w - 1, h])
        if w == 2:
            send(block, block, rz_x.at[1, h], (i, mate * 2 + c), inner)
        send(block, block, rs_x.at[w], (i, sibling))

    gain = gain_ref[...].astype(F32).reshape(1, width)

    def gather(w):
        other, mine = planes[w] * 2 + (1 - c), planes[w] * 2
        arrived(xbuf.at[other], rs_x.at[w])
        for k, b in enumerate(order):
            for t in range(2):
                at = k * TB + t * R
                xn[w, at : at + R, :] = (xbuf[mine + t, b].astype(F32) * gain).astype(BF16)

    def bits():
        for step in range(1, m):
            to = (j + step) % m
            kind = jnp.where(to == sibling, 0, 1)
            send(kw.at[to], kall.at[j], rk.at[0, kind], (i, to))
            send(iown, iall.at[j], rk.at[1, kind], (i, to))

    def expand(rest):
        first, waves = (1, W - 1) if rest else (0, 1)
        arrived(kall.at[0 : m - 2] if rest else kall.at[0], rk.at[0, rest])
        arrived(iall.at[0 : m - 2] if rest else iall.at[0], rk.at[1, rest])
        lanes = kall.shape[2]
        for w in range(first, first + waves):
            for t in range(2):
                at = w * TB + t * R
                word[at : at + R, :] = kall[planes[w] * 2 + t]
                rows_scale[at : at + R, :] = iall[planes[w] * 2 + t]
        lo, high = first * TB, (first + waves) * TB
        packed = word[lo:high, :]
        byte = [jnp.bitwise_and(jnp.right_shift(packed, 8 * q), 255).astype(F32).astype(BF16) for q in range(4)]

        def body(t, carry):
            unit = t * tile + lax.broadcasted_iota(jnp.int32, (lanes, tile), 1)
            where = lax.broadcasted_iota(jnp.int32, (lanes, tile), 0)
            spread_out = jnp.zeros((waves * TB, tile), F32)
            for q in range(4):
                hit = (jnp.right_shift(unit, 3) == where * 4 + q)
                spread_out += jnp.dot(byte[q], jnp.where(hit, 1.0, 0.0).astype(BF16), preferred_element_type=F32)
            shift = jnp.bitwise_and(lax.broadcasted_iota(jnp.int32, (waves * TB, tile), 1), 7)
            bit = jnp.bitwise_and(jnp.right_shift(spread_out.astype(jnp.int32), shift), 1)
            keep[lo:high, pl.ds(pl.multiple_of(t * tile, tile), tile)] = (2 * bit).astype(F32)
            return carry

        lax.fori_loop(0, U // tile, body, 0)

    loaded = [False] * 3

    def ready(k):
        if not loaded[k]:
            loads[k].wait()
        loaded[k] = True

    def project(w, p):
        ready(0)
        ready(1)
        lo, size = parts[w][p]
        at = pl.ds(lo, size)
        for g, wt in enumerate((wg, wu)):

            def body(t, carry):
                cols = pl.ds(pl.multiple_of(t * tile, tile), tile)
                part = jnp.dot(xn[w], wt[:, cols], preferred_element_type=F32)
                direct, kept = (2, 1) if g == 0 else (1, 2)
                pb[w, g, 0, :, cols] = part[0:TB].astype(BF16)
                pb[w, g, 1, :, cols] = part[direct * TB : (direct + 1) * TB].astype(BF16)
                hold[w, g, :, cols] = part[kept * TB : (kept + 1) * TB]
                pown[w, g, :, cols] = part[3 * TB : 4 * TB]
                return carry

            lax.fori_loop(lo // tile, (lo + size) // tile, body, 0)
            to = (xnb, ynb)[g]
            send(pb.at[w, g, 0, :, at], relay.at[w, g, :, at], rp.at[base[w] + p, g], (to, j))
            send(pb.at[w, g, 1, :, at], land.at[w, g, :, at], rp.at[base[w] + p, 2], (to, j))

    def pass_on(w, p, g):
        lo, size = parts[w][p]
        at = pl.ds(lo, size)
        arrived(relay.at[w, g, :, at], rp.at[base[w] + p, g])
        sums[w, g, :, at] = (hold[w, g, :, at] + relay[w, g, :, at].astype(F32)).astype(BF16)
        send(sums.at[w, g, :, at], land.at[w, 2 + g, :, at], rp.at[base[w] + p, 2], ((ynb, xnb)[g], j))

    def activate(w, p):
        lo, size = parts[w][p]
        at = pl.ds(lo, size)
        arrived(land.at[w, :, :, at], rp.at[base[w] + p, 2])
        scale = rows_scale[w * TB : (w + 1) * TB, 0:1]
        gate = (pown[w, 0, :, at] + land[w, 0, :, at].astype(F32) + land[w, 2, :, at].astype(F32)) * scale
        up = (pown[w, 1, :, at] + land[w, 1, :, at].astype(F32) + land[w, 3, :, at].astype(F32)) * scale
        hbuf[w, i, :, at] = (gate / (1.0 + jnp.exp(-gate)) * up * keep[w * TB : (w + 1) * TB, lo : lo + size]).astype(BF16)
        k = len(groups(w)) - 1 if p in groups(w)[-1] else 0
        rest = rh.at[w, k]
        for q, to in enumerate((xnb, ynb)):
            sem = rf.at[base[w] + p] if q == (p + w) % 2 else rest
            send(hbuf.at[w, i, :, at], hbuf.at[w, i, :, at], sem, (to, j))

    def forward(w, p):
        lo, size = parts[w][p]
        at = pl.ds(lo, size)
        src, to = ((xnb, ynb), (ynb, xnb))[(p + w) % 2]
        arrived(hbuf.at[w, src, :, at], rf.at[base[w] + p])
        k = len(groups(w)) - 1 if p in groups(w)[-1] else 0
        send(hbuf.at[w, src, :, at], hbuf.at[w, src, :, at], rh.at[w, k], (to, j))

    def groups(w):
        count = len(parts[w])
        return (range(count - 1), (count - 1,)) if SPLIT_LAST[w] else (range(count),)

    def down(w, k, h):
        ready(2)
        group = groups(w)[k]
        final = k == len(groups(w)) - 1
        low, top = parts[w][group[0]][0], sum(parts[w][group[-1]])
        if h == 0:
            arrived(hbuf.at[w, 0:2, :, pl.ds(low, top - low)], rh.at[w, k])

        def body(t, carry):
            cols = pl.ds(pl.multiple_of(t * tile, tile), tile)
            part = jnp.dot(
                hbuf[w, :, :, low:top].reshape(n * TB, top - low), wd[low:top, cols], preferred_element_type=F32
            )
            for b in range(n):
                for r in range(2):
                    piece = part[b * TB + r * R : b * TB + (r + 1) * R]
                    if k:
                        piece = piece + qf[w, r, b, :, cols]
                    qf[w, r, b, :, cols] = piece
                    if final:
                        qb[w, r, b, :, cols] = piece.astype(BF16)
            return carry

        lax.fori_loop(h * span // tile, (h + 1) * span // tile, body, 0, unroll=True)
        if final:
            at = halves[h]
            send(qb.at[w, 1 - c, :, :, at], sib.at[w, :, :, at], rs.at[w, h], (i, sibling))

    def pair(w, h):
        at, plane = halves[h], planes[w]
        arrived(sib.at[w, :, :, at], rs.at[w, h])
        both = qf[w, c, :, :, at] + sib[w, :, :, at].astype(F32)
        qf[w, c, :, :, at] = both
        ssend[w, :, :, at] = both.astype(BF16)
        send(ssend.at[w, far, :, at], zpass.at[plane, :, at], rpass.at[plane, h], (i, mate * 2 + c), outer)
        send(ssend.at[w, far_end, :, at], zr.at[plane, 1 + within, :, at], rz.at[plane], (i, far_end * 2 + c))
        send(ssend.at[w, mate, :, at], zr.at[plane, 0, :, at], rz.at[plane], (i, mate * 2 + c))

    def join(w, h):
        at = halves[h]
        mine = w if w > 1 else 1 - w
        plane = planes[mine]

        @pl.when(inner)
        def _():
            arrived(zpass.at[plane, :, at], rpass.at[plane, h])
            jsend[w, :, at] = (qf[mine, c, far, :, at] + zpass[plane, :, at].astype(F32)).astype(BF16)

        send(jsend.at[w, :, at], zr.at[plane, 1, :, at], rz.at[plane], (i, far * 2 + c), inner)

    def finish(k):
        w = (2, 1 - within, within, 3)[k]
        plane = (far, mate + within * (z - mate), z + within * (mate - z), far_end)[k]
        @pl.when(outer)
        def _():
            arrived(zr.at[plane], rz.at[plane])

        @pl.when(inner)
        def _():
            arrived(zr.at[plane, 0:2], rz.at[plane])

        value = qf[w, c, z] + zr[plane, 0].astype(F32) + zr[plane, 1].astype(F32)
        qf[w, c, z] = value

        @pl.when(outer)
        def _():
            qf[w, c, z] = qf[w, c, z] + zr[plane, 2].astype(F32)

        result = (xbuf[plane * 2 + c, z].astype(F32) + qf[w, c, z]).astype(BF16)
        wide = result.astype(F32)
        row = pl.multiple_of(plane * TB + c * R, R)
        cown[pl.ds(row, R), :] = jnp.broadcast_to(jnp.sum(wide * wide, axis=1, keepdims=True), (R, cown.shape[1]))
        osend[plane] = result
        here = plane // 2 == c
        slot = plane % 2

        @pl.when(here)
        def _():
            oown[2 * slot + c] = result

        send(osend.at[plane], oown.at[2 * slot + c], ro.at[0], (i, sibling), jnp.logical_not(here))

    table = {
        "own": own, "spread": spread, "ring": ring, "gather": gather, "bits": bits, "expand": expand, "project": project, "relay": pass_on,
        "activate": activate, "forward": forward, "down": down, "pair": pair, "join": join, "finish": finish,
    }
    for name, *step in SCHEDULE:
        table[name](*step)

    csend[...] = jnp.transpose(cown[...])[0:8, :]
    for k, other in enumerate((diag, xnb, ynb)):
        for t in range(2):
            send(csend, call.at[2 * k + c], rc.at[0], (other, z * 2 + t))
    send(csend, call.at[6], rc.at[0], (i, sibling))
    arrived(oown.at[0:2], ro.at[0])
    for q in range(4):
        out_ref[q * R : (q + 1) * R, :] = oown[q]
    arrived(call, rc.at[0])
    check = csend[...]
    for k in range(7):
        check = check + call[k]
    check = check / x_ref.shape[1]
    chk_ref[...] = jnp.where(c == 0, check[0, 0:out_rows], check[0, out_rows : 2 * out_rows])

    for at in range(SENDS):
        settle(at)


def on_plane(saved_input, keep_bits, norm_gain, gate_weight, up_weight, down_weight):
    n, m = lax.axis_size("dp"), lax.axis_size("tensor")
    R, full = saved_input.shape
    width, U = gate_weight.shape
    W = m // 2
    TB = 2 * R
    out_rows = n * R
    lanes = -(-(keep_bits.shape[1] // m) // 128) * 128
    P2 = sum(COL_PARTS)
    dma = pltpu.SemaphoreType.DMA
    vmem = pl.BlockSpec(memory_space=pltpu.VMEM)
    hbm = pl.BlockSpec(memory_space=pl.ANY)
    V = pltpu.VMEM
    scratch = [
        V((R, full), BF16), V(keep_bits.shape, jnp.int32), V((width,), BF16),
        V((width, U), BF16), V((width, U), BF16), V((U, width), BF16),
        V((m, n, R, width), BF16), V((W, n * TB, width), BF16),
        V((m, R, lanes), jnp.int32), V((m, R, lanes), jnp.int32),
        V((R, 128), F32), V((m, R, 128), F32), V((W * TB, lanes), jnp.int32), V((W * TB, 128), F32), V((W * TB, U), F32),
        V((W, 2, 2, TB, U), BF16), V((W, 2, TB, U), F32), V((W, 2, TB, U), F32),
        V((W, 2, TB, U), BF16), V((W, 4, TB, U), BF16), V((W, 2, TB, U), BF16),
        V((W, n, TB, U), BF16),
        V((W, 2, n, R, width), F32), V((W, 2, n, R, width), BF16),
        V((W, n, R, width), BF16), V((W, n, R, width), BF16), V((W, R, width), BF16),
        V((W, 3, R, width), BF16), V((W, R, width), BF16),
        V((n, R, width), BF16), V((W, R, width), BF16),
        V((W * TB, 128), F32), V((8, W * TB), F32), V((7, 8, W * TB), F32),
        dma((3,)), dma((3,)), dma((SENDS,)), dma((2,)), dma((W,)), dma((3, 2)), dma((2, 2)),
        dma((P2, 3)), dma((P2,)), dma((W, 2)), dma((W, 2)), dma((W,)), dma((W, 2)), dma((1,)), dma((1,)),
    ]
    layer_out, check = pl.pallas_call(
        fused,
        out_shape=(
            pltpu.VMEM((out_rows, width), BF16),
            pltpu.VMEM((out_rows,), F32),
        ),
        in_specs=[hbm] * 6,
        out_specs=(vmem, vmem),
        scratch_shapes=scratch,
        compiler_params=pltpu.CompilerParams(
            collective_id=0, has_side_effects=True, vmem_limit_bytes=60 * 1024 * 1024
        ),
    )(saved_input, keep_bits, norm_gain, gate_weight, up_weight, down_weight)
    return layer_out, check


def solution(mesh):
    placed = (
        P(("dp", "tensor"), None),
        P(("dp", "tensor"), None),
        P("dp"),
        P("dp", "tensor"),
        P("dp", "tensor"),
        P("tensor", "dp"),
    )
    plane = mesh.shape["dp"] == 4 and mesh.shape["tensor"] == 2 * mesh.shape["dp"]
    return jax.shard_map(
        on_plane if plane else on_device,
        mesh=mesh,
        in_specs=placed,
        out_specs=(P("tensor", "dp"), P("tensor")),
        check_vma=False,
    )
```
